32 devices in a mesh: group: 2 (over x), expert: 16 (over z, y, core).
Axes of the slice: x: 2, y: 2, z: 4, core: 2. Of those that a mesh axis runs over, the one named last changes fastest.
Arguments:
- query: bfloat16 [32, 2048], P(('group', 'expert')), parts along dimension 0, may hold values from -600 to 600
- key_new: bfloat16 [32, 2048], P(('group', 'expert')), parts along dimension 0, may hold values from -6 to 6
- value_new: bfloat16 [32, 2048], P(('group', 'expert')), parts along dimension 0, may hold values from -6 to 6
- key_cache: bfloat16 [32, 256, 2048], P(('group', 'expert')), parts along dimension 0, may hold values from -6 to 6
- value_cache: bfloat16 [32, 256, 2048], P(('group', 'expert')), parts along dimension 0, may hold values from -6 to 6
- lengths: int32 [32], P(('group', 'expert')), parts along dimension 0, may hold values from 1 to 256
- hidden: bfloat16 [32, 2048], P(('group', 'expert')), parts along dimension 0, may hold values from -6 to 6
- routes: int32 [32], P('group'), parts along dimension 0, may hold values from 0 to 31, as said below
- w_out: bfloat16 [2048, 2048], P(None, 'expert'), may hold values from -0.125 to 0.125
- ln_gain: bfloat16 [2048], replicated, may hold values from 0.099609375 to 1.8984375
- router: bfloat16 [2048, 32], replicated, may hold values from -0.125 to 0.125
- shared_up: bfloat16 [2048, 8192], P(None, 'expert'), may hold values from -0.125 to 0.125
- shared_down: bfloat16 [8192, 2048], P('expert'), may hold values from -0.0625 to 0.0625
- expert_up: bfloat16 [2048, 131072], P(None, 'expert'), may hold values from -0.125 to 0.125
- expert_down: bfloat16 [131072, 2048], P('expert'), may hold values from -0.09375 to 0.09375
Outputs:
- layer_out: bfloat16 [32, 2048], P(('group', 'expert')), parts along dimension 0
The draws below stay inside these ranges and needn't reach their ends.
There are 2 independent parts, one for each index of `group`. The reference program is written for one: setup_inputs(seed, part) draws one part's arguments, and reference() takes and returns one part's arrays. A program takes and returns all parts, laid end to end along the dimension named above; an argument that names none is the same for every part. Nothing has to cross between parts.
Inputs may be any that keep to these rules, and one draw needn't show every extreme that they name: `routes`: no expert is named by more than 2 tokens of the group, and in every draw some expert is named by exactly 2.
All inputs are finite; a program needn't handle non-finite values.
Results may differ from the reference program's by a relative error of at most 0.0085.
Values may be sent and summed in bfloat16 or wider, within the bound.
No kernel may reach another device: no remote copies, remote signals or barrier semaphores. Data moves between devices by JAX's collectives and lax.ppermute only.
A program may use at most 128 MiB of HBM per device.

```python
import math
import jax
import jax.numpy as jnp
from jax import lax

D = 2048
HEADS = 16
HEAD_DIM = 128
FF = 4096
EXPERTS = 32
SHARED_FF = 8192
CACHE = 256
S = 16
CAP = 2


def draw_query(key, part):
    base = jnp.clip(jax.random.normal(key, (S, D), jnp.float32), -6.0, 6.0)
    return base.astype(jnp.bfloat16)


def draw_routes(key, part):
    order_key = jax.random.fold_in(key, 11)
    hot_key = jax.random.fold_in(key, 12)
    second_key = jax.random.fold_in(key, 13)
    count_key = jax.random.fold_in(key, 14)
    shuffle_key = jax.random.fold_in(key, 15)
    offset_key = jax.random.fold_in(key, 16)
    token_order = jax.random.permutation(order_key, S)
    hottest = jax.random.randint(hot_key, (), 0, EXPERTS)
    second = (hottest + 1 + jax.random.randint(second_key, (), 0, EXPERTS - 1)) % EXPERTS
    second_count = jax.random.randint(count_key, (), 1, CAP + 1)
    expert_index = jnp.arange(EXPERTS, dtype=jnp.int32)
    shuffled = jax.random.permutation(shuffle_key, EXPERTS).astype(jnp.int32)
    shuffled = jnp.where(expert_index == hottest, EXPERTS, shuffled)
    shuffled = jnp.where(expert_index == second, EXPERTS + 1, shuffled)
    others = jnp.argsort(shuffled, stable=True).astype(jnp.int32)
    offset = jax.random.randint(offset_key, (), 0, EXPERTS - 2)
    position = jnp.arange(S, dtype=jnp.int32)
    remaining = (position - CAP - second_count + offset) % (EXPERTS - 2)
    chosen = jnp.where(position < CAP, hottest, jnp.where(position < CAP + second_count, second, others[remaining]))
    return jnp.zeros((S,), jnp.int32).at[token_order].set(chosen.astype(jnp.int32))


def place_ends(entries, own_key, smallest, largest):
    shape = entries.shape
    place = [jax.random.randint(jax.random.fold_in(own_key, axis), (), 0, shape[axis]) for axis in range(len(shape))]
    entries = entries.at[tuple(place)].set(smallest)
    longest = shape.index(max(shape))
    place[longest] = (place[longest] + 1) % shape[longest]
    return entries.at[tuple(place)].set(largest)


def block_levels(own_key, shape, pieces, low, top_value):
    loudness = 1.0
    for dim, parts in pieces:
        heights = jax.random.uniform(jax.random.fold_in(jax.random.fold_in(own_key, 6), dim), (parts,), jnp.float32, low / len(pieces), top_value / len(pieces))
        loudness = loudness * jnp.repeat(jnp.exp(heights), shape[dim] // parts).reshape((-1,) + (1,) * (len(shape) - 1 - dim))
    return loudness


def gaussian(stream_key, shape, width, bound, pieces=(), held_as=jnp.bfloat16):
    drawn = jax.random.normal(stream_key, shape, jnp.float32) * width
    if len(pieces) > 0:
        drawn = block_levels(stream_key, shape, pieces, -0.22, 0.18) * drawn
    return jnp.clip(drawn, min=-bound, max=bound).astype(held_as)


def setup_inputs(seed: int = 0, part: int = 0) -> dict:
    keys = jax.random.split(jax.random.key(seed), 16)
    part_splits = jax.random.split(jax.random.fold_in(keys[15], part), 16)
    return {
        "query": draw_query(jax.random.fold_in(jax.random.fold_in(keys[15], part), 71), part),
        "key_new": gaussian(part_splits[1], (S, D), 1.0, 6.0, ((0, 16),)),
        "value_new": gaussian(part_splits[2], (S, D), 1.0, 6.0, ((0, 16),)),
        "key_cache": gaussian(part_splits[3], (S, CACHE, D), 1.0, 6.0, ((0, 16),)),
        "value_cache": gaussian(part_splits[4], (S, CACHE, D), 1.0, 6.0, ((0, 16),)),
        "lengths": place_ends(jax.random.randint(part_splits[5], (S,), 1, CACHE + 1), jax.random.fold_in(part_splits[5], 1), 1, CACHE).astype(jnp.int32),
        "hidden": gaussian(part_splits[6], (S, D), 1.0, 6.0, ((0, 16),)),
        "routes": draw_routes(jax.random.fold_in(jax.random.fold_in(keys[15], part), 71), part),
        "w_out": gaussian(keys[8], (D, D), D ** -0.5, 0.125, ((1, 16),)),
        "ln_gain": jnp.clip(1.0 + 0.18 * jax.random.normal(keys[9], (D,), jnp.float32), 0.099609375, 1.8984375).astype(jnp.bfloat16),
        "router": gaussian(keys[10], (D, EXPERTS), D ** -0.5, 0.125),
        "shared_up": gaussian(keys[11], (D, SHARED_FF), D ** -0.5, 0.125, ((1, 16),)),
        "shared_down": gaussian(keys[12], (SHARED_FF, D), SHARED_FF ** -0.5, 0.0625, ((0, 16),)),
        "expert_up": gaussian(keys[13], (D, EXPERTS * FF), D ** -0.5, 0.125, ((1, 16),)),
        "expert_down": gaussian(keys[14], (EXPERTS * FF, D), FF ** -0.5, 0.09375, ((0, 16),)),
    }


def attend_one(packed):
    query_row, key_rows, value_rows, key_self, value_self, valid = packed
    scale_factor = 1.0 / math.sqrt(HEAD_DIM)
    head_query = query_row.astype(jnp.float32).reshape(HEADS, HEAD_DIM)
    head_keys = key_rows.astype(jnp.float32).reshape(CACHE, HEADS, HEAD_DIM)
    head_values = value_rows.astype(jnp.float32).reshape(CACHE, HEADS, HEAD_DIM)
    scores = jnp.einsum('hd,chd->hc', head_query, head_keys) * scale_factor
    own_score = lax.optimization_barrier(jnp.sum(head_query * key_self.astype(jnp.float32).reshape(HEADS, HEAD_DIM), axis=1)) * scale_factor
    positions = jnp.arange(CACHE, dtype=jnp.int32)
    scores = jnp.where(positions[None, :] < valid, scores, -1e+30)
    top_score = jnp.maximum(lax.optimization_barrier(jnp.max(scores, axis=1)), own_score)
    weights = jnp.exp(scores - top_score[:, None])
    own_weight = jnp.exp(own_score - top_score)
    normalizer = lax.optimization_barrier(jnp.sum(weights, axis=1)) + own_weight
    weights = lax.optimization_barrier((weights / normalizer[:, None]).astype(jnp.bfloat16)).astype(jnp.float32)
    own_weight = lax.optimization_barrier((own_weight / normalizer).astype(jnp.bfloat16)).astype(jnp.float32)
    mixed_values = jnp.einsum('hc,chd->hd', weights, head_values)
    mixed_values = mixed_values + own_weight[:, None] * value_self.astype(jnp.float32).reshape(HEADS, HEAD_DIM)
    return mixed_values.reshape(D).astype(jnp.bfloat16)

def reference(query, key_new, value_new, key_cache, value_cache, lengths, hidden, routes, w_out, ln_gain, router, shared_up, shared_down, expert_up, expert_down):
    attended = lax.map(attend_one, (query, key_cache, value_cache, key_new, value_new, lengths))
    projected = jnp.dot(attended, w_out, preferred_element_type=jnp.float32).astype(jnp.bfloat16)
    projected = lax.optimization_barrier(projected).astype(jnp.float32)
    residual = hidden.astype(jnp.float32) + projected
    centered = residual - lax.optimization_barrier(jnp.mean(residual, axis=1, keepdims=True))
    variance = lax.optimization_barrier(jnp.mean(centered * centered, axis=1, keepdims=True))
    normed = (centered / jnp.sqrt(jnp.maximum(variance, 0.25)) * ln_gain.astype(jnp.float32)).astype(jnp.bfloat16)
    logits = jnp.dot(normed, router, preferred_element_type=jnp.float32)
    expert_ids = jnp.arange(EXPERTS, dtype=jnp.int32)
    chosen = lax.optimization_barrier(jnp.sum(jnp.where(routes[:, None] == expert_ids[None, :], logits, 0.0), axis=1))
    gate_value = jax.nn.sigmoid(chosen)
    shared_hidden = jax.nn.gelu(jnp.dot(normed, shared_up, preferred_element_type=jnp.float32), approximate=True).astype(jnp.bfloat16)
    shared_out = jnp.dot(shared_hidden, shared_down, preferred_element_type=jnp.float32)
    slot_ids = jnp.arange(CAP, dtype=jnp.int32)

    def one_expert(running, expert_id):
        member = routes == expert_id
        slot_rank = jnp.cumsum(member.astype(jnp.int32)) - 1
        placed = member[:, None] & (slot_rank[:, None] == slot_ids[None, :])
        picked = jnp.dot(placed.astype(jnp.bfloat16).T, normed, preferred_element_type=jnp.float32).astype(jnp.bfloat16)
        up_cols = lax.dynamic_slice_in_dim(expert_up, (expert_id * FF).astype(jnp.int32), FF, 1)
        down_rows = lax.dynamic_slice_in_dim(expert_down, (expert_id * FF).astype(jnp.int32), FF, 0)
        inner_act = jax.nn.gelu(jnp.dot(picked, up_cols, preferred_element_type=jnp.float32), approximate=True).astype(jnp.bfloat16)
        result = jnp.dot(inner_act, down_rows, preferred_element_type=jnp.float32)
        spread = placed.astype(jnp.float32) * gate_value[:, None]
        return (running + jnp.dot(spread, result, precision=lax.Precision.HIGHEST), None)
    expert_out, ignored = lax.scan(one_expert, jnp.zeros((S, D), jnp.float32), expert_ids)
    return (residual + shared_out + expert_out).astype(jnp.bfloat16)
```

```python
import functools
import math

import jax
import jax.numpy as jnp
from jax import lax
from jax.experimental import pallas as pl
from jax.experimental.pallas import tpu as pltpu
from jax.sharding import PartitionSpec as P

D = 2048
HEADS = 16
HEAD_DIM = 128
FF = 4096
EXPERTS = 32


def attend(query, key_new, value_new, key_cache, value_cache, lengths):
    seq_count = query.shape[0]
    cache_len = key_cache.shape[1]
    scale_factor = 1.0 / math.sqrt(HEAD_DIM)
    head_query = query.reshape(seq_count, HEADS, HEAD_DIM)
    head_keys = key_cache.reshape(seq_count, cache_len, HEADS, HEAD_DIM)
    head_values = value_cache.reshape(seq_count, cache_len, HEADS, HEAD_DIM)
    scores = (
        jnp.einsum("shd,schd->shc", head_query, head_keys, preferred_element_type=jnp.float32)
        * scale_factor
    )
    own_score = (
        jnp.einsum(
            "shd,shd->sh",
            head_query,
            key_new.reshape(seq_count, HEADS, HEAD_DIM),
            preferred_element_type=jnp.float32,
        )
        * scale_factor
    )
    positions = jnp.arange(cache_len, dtype=jnp.int32)
    scores = jnp.where(positions[None, None, :] < lengths[:, None, None], scores, -1e30)
    top_score = jnp.maximum(jnp.max(scores, axis=2), own_score)
    weights = jnp.exp(scores - top_score[:, :, None])
    own_weight = jnp.exp(own_score - top_score)
    normalizer = jnp.sum(weights, axis=2) + own_weight
    weights = (weights / normalizer[:, :, None]).astype(jnp.bfloat16)
    own_weight = (own_weight / normalizer).astype(jnp.bfloat16)
    mixed_values = jnp.einsum(
        "shc,schd->shd", weights, head_values, preferred_element_type=jnp.float32
    )
    mixed_values = mixed_values + own_weight.astype(jnp.float32)[:, :, None] * value_new.reshape(
        seq_count, HEADS, HEAD_DIM
    ).astype(jnp.float32)
    return mixed_values.reshape(seq_count, HEADS * HEAD_DIM).astype(jnp.bfloat16)


def body(
    query,
    key_new,
    value_new,
    key_cache,
    value_cache,
    lengths,
    hidden,
    routes,
    w_out,
    ln_gain,
    router,
    shared_up,
    shared_down,
    expert_up,
    expert_down,
):
    seq_count = query.shape[0]
    attended = attend(query, key_new, value_new, key_cache, value_cache, lengths)
    every_attended, every_hidden = (
        lax.all_gather(attended, "expert", axis=0, tiled=True),
        lax.all_gather(hidden, "expert", axis=0, tiled=True),
    )
    projected = jnp.dot(every_attended, w_out, preferred_element_type=jnp.float32).astype(
        jnp.bfloat16
    )
    every_projected = lax.all_gather(projected, "expert", axis=1, tiled=True)
    residual = every_hidden.astype(jnp.float32) + every_projected.astype(jnp.float32)
    centered = residual - jnp.mean(residual, axis=1, keepdims=True)
    variance = jnp.mean(centered * centered, axis=1, keepdims=True)
    normed = (
        centered / jnp.sqrt(jnp.maximum(variance, 0.25)) * ln_gain.astype(jnp.float32)
    ).astype(jnp.bfloat16)
    logits = jnp.dot(normed, router, preferred_element_type=jnp.float32)
    all_experts = jnp.arange(EXPERTS, dtype=jnp.int32)
    chosen = jnp.sum(jnp.where(routes[:, None] == all_experts[None, :], logits, 0.0), axis=1)
    gate_value = jax.nn.sigmoid(chosen)
    shared_hidden = jax.nn.gelu(
        jnp.dot(normed, shared_up, preferred_element_type=jnp.float32), approximate=True
    ).astype(jnp.bfloat16)
    total_tokens = routes.shape[0]
    capacity = 4 * total_tokens // EXPERTS
    column_count = expert_up.shape[1]
    local_units = min(column_count, FF)
    local_experts = column_count // local_units
    device_index = lax.axis_index("expert")
    first_expert = device_index * column_count // FF
    expert_ids = first_expert + jnp.arange(local_experts, dtype=jnp.int32)
    member = routes[:, None] == expert_ids[None, :]
    slot_rank = jnp.cumsum(member.astype(jnp.int32), axis=0) - 1
    slot_ids = jnp.arange(capacity, dtype=jnp.int32)
    placed = member[:, :, None] & (slot_rank[:, :, None] == slot_ids[None, None, :])
    picked = jnp.einsum(
        "skc,sd->kcd", placed.astype(jnp.bfloat16), normed, preferred_element_type=jnp.float32
    ).astype(jnp.bfloat16)
    up_local = expert_up.reshape(D, local_experts, local_units)
    inner_act = jax.nn.gelu(
        jnp.einsum("kcd,dkf->kcf", picked, up_local, preferred_element_type=jnp.float32),
        approximate=True,
    ).astype(jnp.bfloat16)
    down_local = expert_down.reshape(local_experts, local_units, D)
    result = jnp.einsum("kcf,kfd->kcd", inner_act, down_local, preferred_element_type=jnp.float32)
    spread = placed.astype(jnp.float32) * gate_value[:, None, None]
    summed = lax.psum_scatter(
        jnp.dot(shared_hidden, shared_down, preferred_element_type=jnp.float32)
        + jnp.einsum("skc,kcd->sd", spread, result, precision=lax.Precision.HIGHEST),
        "expert",
        scatter_dimension=0,
        tiled=True,
    )
    own_residual = lax.dynamic_slice_in_dim(residual, device_index * seq_count, seq_count, 0)
    combined = own_residual + summed
    return combined.astype(jnp.bfloat16)


LANES = 128


def per_head(row, heads):
    index = lax.broadcasted_iota(jnp.int32, (heads, LANES), 0)
    out = jnp.zeros((heads, LANES), jnp.float32)
    for head in range(heads):
        piece = row[:, head * LANES : (head + 1) * LANES]
        out = jnp.where(index == head, piece, out)
    return out


def attend_kernel(
    lengths, query, key_new, value_new, keys, values, hidden, out,
    query_buf, key_new_buf, value_new_buf, hidden_buf, keys_buf, values_buf, sems,
):
    copies = [
        pltpu.make_async_copy(source, target, sems.at[slot])
        for slot, (source, target) in enumerate(
            (
                (query, query_buf),
                (keys.at[0], keys_buf),
                (key_new, key_new_buf),
                (values.at[0], values_buf),
                (value_new, value_new_buf),
                (hidden, hidden_buf),
            )
        )
    ]
    for copy in copies:
        copy.start()
    cache_len, width = keys_buf.shape
    heads = width // HEAD_DIM
    scale_factor = 1.0 / math.sqrt(HEAD_DIM)
    valid = lengths[0]
    copies[0].wait()
    lane_head = lax.broadcasted_iota(jnp.int32, (heads, width), 1) // HEAD_DIM
    row_head = lax.broadcasted_iota(jnp.int32, (heads, width), 0)
    head_query = jnp.where(lane_head == row_head, query_buf[...].astype(jnp.float32), 0.0)
    copies[2].wait()
    own_score = (
        jnp.sum(head_query * key_new_buf[...].astype(jnp.float32), axis=1, keepdims=True)
        * scale_factor
    )
    copies[1].wait()
    scores = (
        lax.dot_general(
            head_query.astype(jnp.bfloat16),
            keys_buf[...],
            (((1,), (1,)), ((), ())),
            preferred_element_type=jnp.float32,
        )
        * scale_factor
    )
    positions = lax.broadcasted_iota(jnp.int32, (heads, cache_len), 1)
    scores = jnp.where(positions < valid, scores, -1e30)
    top_score = jnp.maximum(jnp.max(scores, axis=1, keepdims=True), own_score)
    weights = jnp.exp(scores - top_score)
    own_weight = jnp.exp(own_score - top_score)
    normalizer = jnp.sum(weights, axis=1, keepdims=True) + own_weight
    weights = (weights / normalizer).astype(jnp.bfloat16)
    own_weight = (own_weight / normalizer).astype(jnp.bfloat16).astype(jnp.float32)
    copies[3].wait()
    mixed = jnp.dot(weights, values_buf[...], preferred_element_type=jnp.float32)
    copies[4].wait()
    copies[5].wait()
    own_value = per_head(value_new_buf[...].astype(jnp.float32), heads)
    attended = (per_head(mixed, heads) + own_weight * own_value).astype(jnp.bfloat16)
    residual = per_head(hidden_buf[...].astype(jnp.float32), heads).astype(jnp.bfloat16)
    message = jnp.concatenate([attended, residual], axis=0)
    out[...] = jnp.broadcast_to(message[None], out.shape)


def project_kernel(gathered, w_out, out, hidden_out):
    tokens, rows, _ = gathered.shape
    total = tokens * rows
    flat = gathered[...].reshape(total, LANES)
    target = lax.broadcasted_iota(jnp.int32, (total, total), 0)
    source = lax.broadcasted_iota(jnp.int32, (total, total), 1)
    wanted = (target % tokens) * rows + target // tokens
    swap = jnp.where(source == wanted, 1.0, 0.0).astype(jnp.bfloat16)
    swapped = jnp.dot(swap, flat, preferred_element_type=jnp.float32).astype(jnp.bfloat16)
    blocks = [swapped[row * tokens : (row + 1) * tokens] for row in range(rows)]
    attended = jnp.concatenate(blocks[: rows // 2], axis=1)
    hidden_out[...] = jnp.concatenate(blocks[rows // 2 :], axis=1)
    projected = jnp.dot(attended, w_out[...], preferred_element_type=jnp.float32)
    out[...] = jnp.broadcast_to(projected.astype(jnp.bfloat16)[None], out.shape)


def gelu(value):
    return jax.nn.gelu(value, approximate=True).astype(jnp.bfloat16)


def mlp_kernel(
    axis, local_experts, up_step, down_step, slots,
    routes, projected, hidden, ln_gain, router, shared_up, shared_down, expert_up, expert_down,
    out, own_out,
    router_buf, shared_up_buf, shared_down_buf, down_buf, act_buf, sems, down_sems,
):
    device_index = lax.axis_index(axis)
    tokens, width = hidden.shape
    columns = expert_up.shape[1]
    units = columns // local_experts
    down_count = columns // down_step

    def down_copy(index):
        slot = lax.rem(index, slots)
        return pltpu.make_async_copy(
            expert_down.at[pl.ds(pl.multiple_of(index * down_step, down_step), down_step)],
            down_buf.at[slot],
            down_sems.at[slot],
        )

    router_copy = pltpu.make_async_copy(router, router_buf, sems.at[0])
    shared_up_copy = pltpu.make_async_copy(shared_up, shared_up_buf, sems.at[1])
    shared_down_copy = pltpu.make_async_copy(shared_down, shared_down_buf, sems.at[2])
    shared_up_copy.start()
    router_copy.start()
    shared_down_copy.start()
    for index in range(min(slots, down_count)):
        down_copy(index).start()

    blocks = width // LANES
    every_projected = jnp.concatenate(
        [projected[block].astype(jnp.float32) for block in range(projected.shape[0])], axis=1
    )
    residual = hidden[...].astype(jnp.float32) + every_projected
    token = lax.broadcasted_iota(jnp.int32, (tokens, width), 0)
    own = jnp.sum(jnp.where(token == device_index, residual, 0.0), axis=0, keepdims=True)
    own_out[...] = per_head(own, blocks)
    centered = residual - jnp.mean(residual, axis=1, keepdims=True)
    variance = jnp.mean(centered * centered, axis=1, keepdims=True)
    gain = ln_gain[...].astype(jnp.float32)
    gain = jnp.concatenate([gain[block : block + 1] for block in range(blocks)], axis=1)
    normed = (centered / jnp.sqrt(jnp.maximum(variance, 0.25)) * gain).astype(jnp.bfloat16)

    def up_body(step, carry):
        at = pl.ds(pl.multiple_of(step * up_step, up_step), up_step)
        act_buf[:, at] = gelu(
            jnp.dot(normed, expert_up[:, at], preferred_element_type=jnp.float32)
        )
        return carry

    lax.fori_loop(0, columns // up_step, up_body, 0)

    router_copy.wait()
    logits = lax.dot_general(
        normed, router_buf[...], (((1,), (1,)), ((), ())), preferred_element_type=jnp.float32
    )
    experts = logits.shape[1]
    token_column = lax.broadcasted_iota(jnp.int32, (tokens, 1), 0)
    route = jnp.zeros((tokens, 1), jnp.int32)
    for index in range(tokens):
        route = jnp.where(token_column == index, routes[index], route)
    expert_lane = lax.broadcasted_iota(jnp.int32, (tokens, experts), 1)
    chosen = jnp.sum(jnp.where(expert_lane == route, logits, 0.0), axis=1, keepdims=True)
    gate = jax.nn.sigmoid(chosen)
    shared_up_copy.wait()
    shared_act = gelu(jnp.dot(normed, shared_up_buf[...], preferred_element_type=jnp.float32))
    shared_down_copy.wait()
    total = jnp.dot(shared_act, shared_down_buf[...], preferred_element_type=jnp.float32)

    for expert in range(local_experts):
        first = expert * (units // down_step)

        def down_body(step, sums):
            index = first + step
            slot = lax.rem(index, slots)
            down_copy(index).wait()
            at = pl.ds(pl.multiple_of(index * down_step, down_step), down_step)
            sums = sums + jnp.dot(
                act_buf[:, at], down_buf[slot], preferred_element_type=jnp.float32
            )

            @pl.when(index + slots < down_count)
            def _():
                down_copy(index + slots).start()

            return sums

        sums = lax.fori_loop(
            0, units // down_step, down_body, jnp.zeros((tokens, width), jnp.float32)
        )
        here = route == device_index * local_experts + expert
        total = total + jnp.where(here, gate, 0.0) * sums

    for block in range(blocks):
        out[:, block, :] = total[:, block * LANES : (block + 1) * LANES]


def combine_kernel(terms, own, out):
    total = own[...]
    for index in range(terms.shape[0]):
        total = total + terms[index]
    for block in range(total.shape[0]):
        out[:, block * LANES : (block + 1) * LANES] = total[block : block + 1].astype(out.dtype)


VMEM = pl.BlockSpec(memory_space=pltpu.VMEM)
SMEM = pl.BlockSpec(memory_space=pltpu.SMEM)
HBM = pl.BlockSpec(memory_space=pltpu.HBM)


def params(megabytes):
    return pltpu.CompilerParams(vmem_limit_bytes=megabytes << 20)


def cost(flops):
    return pl.CostEstimate(flops=flops, bytes_accessed=flops >> 8, transcendentals=0)


def fast_body(
    query, key_new, value_new, key_cache, value_cache, lengths, hidden, routes, w_out,
    ln_gain, router, shared_up, shared_down, expert_up, expert_down,
):
    width = query.shape[1]
    blocks = width // LANES
    cache_len = key_cache.shape[1]
    tokens = routes.shape[0]
    columns = expert_up.shape[1]
    in_hbm = functools.partial(pltpu.with_memory_space_constraint, memory_space=pltpu.HBM)
    query, key_new, value_new, key_cache, value_cache, hidden = map(
        in_hbm, (query, key_new, value_new, key_cache, value_cache, hidden)
    )
    router, shared_up, shared_down, expert_down = map(
        in_hbm, (router.T, shared_up, shared_down, expert_down)
    )
    expert_up = pltpu.with_memory_space_constraint(expert_up, pltpu.VMEM)
    row = pltpu.VMEM((1, width), jnp.bfloat16)
    cache = pltpu.VMEM((cache_len, width), jnp.bfloat16)
    message = pl.pallas_call(
        attend_kernel,
        out_shape=jax.ShapeDtypeStruct((tokens, 2 * blocks, LANES), jnp.bfloat16),
        in_specs=[SMEM] + [HBM] * 6,
        out_specs=VMEM,
        scratch_shapes=[row] * 4 + [cache] * 2 + [pltpu.SemaphoreType.DMA((6,))],
        compiler_params=params(4),
        cost_estimate=cost(10**11),
        name="attend",
    )(lengths, query, key_new, value_new, key_cache, value_cache, hidden)
    gathered = lax.all_to_all(message, "expert", 0, 0)
    message, every_hidden = pl.pallas_call(
        project_kernel,
        out_shape=(
            jax.ShapeDtypeStruct((tokens, tokens, LANES), jnp.bfloat16),
            jax.ShapeDtypeStruct((tokens, width), jnp.bfloat16),
        ),
        in_specs=[VMEM] * 2,
        out_specs=(VMEM, VMEM),
        compiler_params=params(4),
        cost_estimate=cost(10**11),
        name="project",
    )(gathered, w_out)
    every_projected = lax.all_to_all(message, "expert", 0, 0)
    local_experts = columns // FF
    slots, down_step, up_step = 11, 512, 1024
    terms, own = pl.pallas_call(
        functools.partial(mlp_kernel, "expert", local_experts, up_step, down_step, slots),
        out_shape=(
            jax.ShapeDtypeStruct((tokens, blocks, LANES), jnp.float32),
            jax.ShapeDtypeStruct((blocks, LANES), jnp.float32),
        ),
        in_specs=[SMEM, VMEM, VMEM, VMEM, HBM, HBM, HBM, VMEM, HBM],
        out_specs=(VMEM, VMEM),
        scratch_shapes=[
            pltpu.VMEM(router.shape, router.dtype),
            pltpu.VMEM(shared_up.shape, shared_up.dtype),
            pltpu.VMEM(shared_down.shape, shared_down.dtype),
            pltpu.VMEM((slots, down_step, width), expert_down.dtype),
            pltpu.VMEM((tokens, columns), jnp.bfloat16),
            pltpu.SemaphoreType.DMA((3,)),
            pltpu.SemaphoreType.DMA((slots,)),
        ],
        compiler_params=params(29),
        cost_estimate=cost(10**11),
        name="mlp",
    )(
        routes, every_projected, every_hidden, ln_gain.reshape(blocks, LANES), router,
        shared_up, shared_down, expert_up, expert_down,
    )
    terms = lax.all_to_all(terms, "expert", 0, 0)
    return pl.pallas_call(
        combine_kernel,
        out_shape=jax.ShapeDtypeStruct((1, width), jnp.bfloat16),
        in_specs=[VMEM] * 2,
        out_specs=VMEM,
        compiler_params=params(2),
        name="combine",
    )(terms, own)


def fits_fast(
    query, key_new, value_new, key_cache, value_cache, lengths, hidden, routes, w_out, *rest
):
    tokens = routes.shape[0]
    return (
        query.shape[0] == 1
        and HEAD_DIM == LANES
        and w_out.shape[1] == LANES
        and tokens * LANES == query.shape[1]
        and rest[4].shape[1] % FF == 0
    )


def pick_body(*args):
    return fast_body(*args) if fits_fast(*args) else body(*args)


def solution(mesh):
    placed = (
        P(("group", "expert"), None),
        P(("group", "expert"), None),
        P(("group", "expert"), None),
        P(("group", "expert"), None, None),
        P(("group", "expert"), None, None),
        P(("group", "expert")),
        P(("group", "expert"), None),
        P("group"),
        P(None, "expert"),
        P(),
        P(),
        P(None, "expert"),
        P("expert", None),
        P(None, "expert"),
        P("expert", None),
    )
    return jax.shard_map(
        pick_body, mesh=mesh, in_specs=placed, out_specs=P(("group", "expert"), None), check_vma=False
    )
```

```python
import functools
import math

import jax
import jax.numpy as jnp
from jax import lax
from jax.experimental import pallas as pl
from jax.experimental.pallas import tpu as pltpu
from jax.sharding import PartitionSpec as P

D = 2048
HEADS = 16
HEAD_DIM = 128
FF = 4096
EXPERTS = 32


def attend(query, key_new, value_new, key_cache, value_cache, lengths):
    seq_count = query.shape[0]
    cache_len = key_cache.shape[1]
    scale_factor = 1.0 / math.sqrt(HEAD_DIM)
    head_query = query.reshape(seq_count, HEADS, HEAD_DIM)
    head_keys = key_cache.reshape(seq_count, cache_len, HEADS, HEAD_DIM)
    head_values = value_cache.reshape(seq_count, cache_len, HEADS, HEAD_DIM)
    scores = (
        jnp.einsum("shd,schd->shc", head_query, head_keys, preferred_element_type=jnp.float32)
        * scale_factor
    )
    own_score = (
        jnp.einsum(
            "shd,shd->sh",
            head_query,
            key_new.reshape(seq_count, HEADS, HEAD_DIM),
            preferred_element_type=jnp.float32,
        )
        * scale_factor
    )
    positions = jnp.arange(cache_len, dtype=jnp.int32)
    scores = jnp.where(positions[None, None, :] < lengths[:, None, None], scores, -1e30)
    top_score = jnp.maximum(jnp.max(scores, axis=2), own_score)
    weights = jnp.exp(scores - top_score[:, :, None])
    own_weight = jnp.exp(own_score - top_score)
    normalizer = jnp.sum(weights, axis=2) + own_weight
    weights = (weights / normalizer[:, :, None]).astype(jnp.bfloat16)
    own_weight = (own_weight / normalizer).astype(jnp.bfloat16)
    mixed_values = jnp.einsum(
        "shc,schd->shd", weights, head_values, preferred_element_type=jnp.float32
    )
    mixed_values = mixed_values + own_weight.astype(jnp.float32)[:, :, None] * value_new.reshape(
        seq_count, HEADS, HEAD_DIM
    ).astype(jnp.float32)
    return mixed_values.reshape(seq_count, HEADS * HEAD_DIM).astype(jnp.bfloat16)


def body(
    query,
    key_new,
    value_new,
    key_cache,
    value_cache,
    lengths,
    hidden,
    routes,
    w_out,
    ln_gain,
    router,
    shared_up,
    shared_down,
    expert_up,
    expert_down,
):
    seq_count = query.shape[0]
    attended = attend(query, key_new, value_new, key_cache, value_cache, lengths)
    every_attended, every_hidden = (
        lax.all_gather(attended, "expert", axis=0, tiled=True),
        lax.all_gather(hidden, "expert", axis=0, tiled=True),
    )
    projected = jnp.dot(every_attended, w_out, preferred_element_type=jnp.float32).astype(
        jnp.bfloat16
    )
    every_projected = lax.all_gather(projected, "expert", axis=1, tiled=True)
    residual = every_hidden.astype(jnp.float32) + every_projected.astype(jnp.float32)
    centered = residual - jnp.mean(residual, axis=1, keepdims=True)
    variance = jnp.mean(centered * centered, axis=1, keepdims=True)
    normed = (
        centered / jnp.sqrt(jnp.maximum(variance, 0.25)) * ln_gain.astype(jnp.float32)
    ).astype(jnp.bfloat16)
    logits = jnp.dot(normed, router, preferred_element_type=jnp.float32)
    all_experts = jnp.arange(EXPERTS, dtype=jnp.int32)
    chosen = jnp.sum(jnp.where(routes[:, None] == all_experts[None, :], logits, 0.0), axis=1)
    gate_value = jax.nn.sigmoid(chosen)
    shared_hidden = jax.nn.gelu(
        jnp.dot(normed, shared_up, preferred_element_type=jnp.float32), approximate=True
    ).astype(jnp.bfloat16)
    total_tokens = routes.shape[0]
    capacity = 4 * total_tokens // EXPERTS
    column_count = expert_up.shape[1]
    local_units = min(column_count, FF)
    local_experts = column_count // local_units
    device_index = lax.axis_index("expert")
    first_expert = device_index * column_count // FF
    expert_ids = first_expert + jnp.arange(local_experts, dtype=jnp.int32)
    member = routes[:, None] == expert_ids[None, :]
    slot_rank = jnp.cumsum(member.astype(jnp.int32), axis=0) - 1
    slot_ids = jnp.arange(capacity, dtype=jnp.int32)
    placed = member[:, :, None] & (slot_rank[:, :, None] == slot_ids[None, None, :])
    picked = jnp.einsum(
        "skc,sd->kcd", placed.astype(jnp.bfloat16), normed, preferred_element_type=jnp.float32
    ).astype(jnp.bfloat16)
    up_local = expert_up.reshape(D, local_experts, local_units)
    inner_act = jax.nn.gelu(
        jnp.einsum("kcd,dkf->kcf", picked, up_local, preferred_element_type=jnp.float32),
        approximate=True,
    ).astype(jnp.bfloat16)
    down_local = expert_down.reshape(local_experts, local_units, D)
    result = jnp.einsum("kcf,kfd->kcd", inner_act, down_local, preferred_element_type=jnp.float32)
    spread = placed.astype(jnp.float32) * gate_value[:, None, None]
    summed = lax.psum_scatter(
        jnp.dot(shared_hidden, shared_down, preferred_element_type=jnp.float32)
        + jnp.einsum("skc,kcd->sd", spread, result, precision=lax.Precision.HIGHEST),
        "expert",
        scatter_dimension=0,
        tiled=True,
    )
    own_residual = lax.dynamic_slice_in_dim(residual, device_index * seq_count, seq_count, 0)
    combined = own_residual + summed
    return combined.astype(jnp.bfloat16)


LANES = 128


def per_head(row, heads):
    index = lax.broadcasted_iota(jnp.int32, (heads, LANES), 0)
    out = jnp.zeros((heads, LANES), jnp.float32)
    for head in range(heads):
        piece = row[:, head * LANES : (head + 1) * LANES]
        out = jnp.where(index == head, piece, out)
    return out


def attend_kernel(
    lengths, query, key_new, value_new, keys, values, hidden, out,
    query_buf, key_new_buf, value_new_buf, hidden_buf, keys_buf, values_buf, sems,
):
    copies = [
        pltpu.make_async_copy(source, target, sems.at[slot])
        for slot, (source, target) in enumerate(
            (
                (query, query_buf),
                (keys.at[0], keys_buf),
                (key_new, key_new_buf),
                (values.at[0], values_buf),
                (value_new, value_new_buf),
                (hidden, hidden_buf),
            )
        )
    ]
    for copy in copies:
        copy.start()
    cache_len, width = keys_buf.shape
    heads = width // HEAD_DIM
    scale_factor = 1.0 / math.sqrt(HEAD_DIM)
    valid = lengths[0]
    copies[0].wait()
    lane_head = lax.broadcasted_iota(jnp.int32, (heads, width), 1) // HEAD_DIM
    row_head = lax.broadcasted_iota(jnp.int32, (heads, width), 0)
    head_query = jnp.where(lane_head == row_head, query_buf[...].astype(jnp.float32), 0.0)
    copies[2].wait()
    own_score = (
        jnp.sum(head_query * key_new_buf[...].astype(jnp.float32), axis=1, keepdims=True)
        * scale_factor
    )
    copies[1].wait()
    scores = (
        lax.dot_general(
            head_query.astype(jnp.bfloat16),
            keys_buf[...],
            (((1,), (1,)), ((), ())),
            preferred_element_type=jnp.float32,
        )
        * scale_factor
    )
    positions = lax.broadcasted_iota(jnp.int32, (heads, cache_len), 1)
    scores = jnp.where(positions < valid, scores, -1e30)
    top_score = jnp.maximum(jnp.max(scores, axis=1, keepdims=True), own_score)
    weights = jnp.exp(scores - top_score)
    own_weight = jnp.exp(own_score - top_score)
    normalizer = jnp.sum(weights, axis=1, keepdims=True) + own_weight
    weights = (weights / normalizer).astype(jnp.bfloat16)
    own_weight = (own_weight / normalizer).astype(jnp.bfloat16).astype(jnp.float32)
    copies[3].wait()
    mixed = jnp.dot(weights, values_buf[...], preferred_element_type=jnp.float32)
    copies[4].wait()
    copies[5].wait()
    own_value = per_head(value_new_buf[...].astype(jnp.float32), heads)
    attended = (per_head(mixed, heads) + own_weight * own_value).astype(jnp.bfloat16)
    residual = per_head(hidden_buf[...].astype(jnp.float32), heads).astype(jnp.bfloat16)
    message = jnp.concatenate([attended, residual], axis=0)
    out[...] = jnp.broadcast_to(message[None], out.shape)


def project_kernel(gathered, w_out, shared_up, shared_down, out, hidden_out):
    tokens, rows, _ = gathered.shape
    total = tokens * rows
    flat = gathered[...].reshape(total, LANES)
    target = lax.broadcasted_iota(jnp.int32, (total, total), 0)
    source = lax.broadcasted_iota(jnp.int32, (total, total), 1)
    wanted = (target % tokens) * rows + target // tokens
    swap = jnp.where(source == wanted, 1.0, 0.0).astype(jnp.bfloat16)
    swapped = jnp.dot(swap, flat, preferred_element_type=jnp.float32).astype(jnp.bfloat16)
    blocks = [swapped[row * tokens : (row + 1) * tokens] for row in range(rows)]
    attended = jnp.concatenate(blocks[: rows // 2], axis=1)
    hidden_out[...] = jnp.concatenate(blocks[rows // 2 :], axis=1)
    projected = jnp.dot(attended, w_out[...], preferred_element_type=jnp.float32)
    out[...] = jnp.broadcast_to(projected.astype(jnp.bfloat16)[None], out.shape)


def gelu(value):
    return jax.nn.gelu(value, approximate=True).astype(jnp.bfloat16)


def mlp_kernel(
    axis, local_experts, up_step, down_step, slots,
    routes, projected, hidden, ln_gain, router, shared_up, shared_down, expert_up, expert_down,
    out, own_out,
    router_buf, down_buf, act_buf, router_sem, down_sems,
):
    device_index = lax.axis_index(axis)
    tokens, width = hidden.shape
    columns = expert_up.shape[1]
    units = columns // local_experts
    down_count = columns // down_step

    def down_copy(index):
        slot = index % slots
        return pltpu.make_async_copy(
            expert_down.at[index * down_step : (index + 1) * down_step],
            down_buf.at[slot],
            down_sems.at[slot],
        )

    router_copy = pltpu.make_async_copy(router, router_buf, router_sem)
    router_copy.start()
    for index in range(min(slots, down_count)):
        down_copy(index).start()

    blocks = width // LANES
    every_projected = jnp.concatenate(
        [projected[block].astype(jnp.float32) for block in range(projected.shape[0])], axis=1
    )
    residual = hidden[...].astype(jnp.float32) + every_projected
    token = lax.broadcasted_iota(jnp.int32, (tokens, width), 0)
    own = jnp.sum(jnp.where(token == device_index, residual, 0.0), axis=0, keepdims=True)
    own_out[...] = per_head(own, blocks)
    centered = residual - jnp.mean(residual, axis=1, keepdims=True)
    variance = jnp.mean(centered * centered, axis=1, keepdims=True)
    gain = ln_gain[...].astype(jnp.float32)
    gain = jnp.concatenate([gain[block : block + 1] for block in range(blocks)], axis=1)
    normed = (centered / jnp.sqrt(jnp.maximum(variance, 0.25)) * gain).astype(jnp.bfloat16)

    router_copy.wait()
    logits = lax.dot_general(
        normed, router_buf[...], (((1,), (1,)), ((), ())), preferred_element_type=jnp.float32
    )
    experts = logits.shape[1]
    token_column = lax.broadcasted_iota(jnp.int32, (tokens, 1), 0)
    route = jnp.zeros((tokens, 1), jnp.int32)
    for index in range(tokens):
        route = jnp.where(token_column == index, routes[index], route)
    expert_lane = lax.broadcasted_iota(jnp.int32, (tokens, experts), 1)
    chosen = jnp.sum(jnp.where(expert_lane == route, logits, 0.0), axis=1, keepdims=True)
    gate = jax.nn.sigmoid(chosen)
    shared_act = gelu(jnp.dot(normed, shared_up[...], preferred_element_type=jnp.float32))
    total = jnp.dot(shared_act, shared_down[...], preferred_element_type=jnp.float32)

    for expert in range(local_experts):
        first = expert * (units // down_step)

        for step in range(expert * units // up_step, (expert + 1) * units // up_step):
            at = slice(step * up_step, (step + 1) * up_step)
            act_buf[:, at] = gelu(
                jnp.dot(normed, expert_up[:, at], preferred_element_type=jnp.float32)
            )
        sums = jnp.zeros((tokens, width), jnp.float32)
        for index in range(first, first + units // down_step):
            down_copy(index).wait()
            at = slice(index * down_step, (index + 1) * down_step)
            sums = sums + jnp.dot(
                act_buf[:, at], down_buf[index % slots], preferred_element_type=jnp.float32
            )
            if index + slots < down_count:
                down_copy(index + slots).start()
        here = route == device_index * local_experts + expert
        total = total + jnp.where(here, gate, 0.0) * sums

    for block in range(blocks):
        out[:, block, :] = total[:, block * LANES : (block + 1) * LANES]


def combine_kernel(terms, own, out):
    total = own[...]
    for index in range(terms.shape[0]):
        total = total + terms[index]
    for block in range(total.shape[0]):
        out[:, block * LANES : (block + 1) * LANES] = total[block : block + 1].astype(out.dtype)


VMEM = pl.BlockSpec(memory_space=pltpu.VMEM)
SMEM = pl.BlockSpec(memory_space=pltpu.SMEM)
HBM = pl.BlockSpec(memory_space=pltpu.HBM)


def params(megabytes):
    return pltpu.CompilerParams(vmem_limit_bytes=megabytes << 20)


def cost(flops):
    return pl.CostEstimate(flops=flops, bytes_accessed=flops >> 8, transcendentals=0)


def mlp(
    routes, projected, hidden, ln_gain, router, shared_up, shared_down, expert_up, expert_down
):
    tokens, width = hidden.shape
    blocks = width // LANES
    columns = expert_up.shape[1]
    local_experts = columns // FF
    slots, down_step, up_step = 9, 512, 1024
    return pl.pallas_call(
        functools.partial(mlp_kernel, "expert", local_experts, up_step, down_step, slots),
        out_shape=(
            pltpu.VMEM((tokens, blocks, LANES), jnp.float32),
            pltpu.VMEM((blocks, LANES), jnp.float32),
        ),
        in_specs=[SMEM, VMEM, VMEM, VMEM, HBM, VMEM, VMEM, VMEM, HBM],
        out_specs=(VMEM, VMEM),
        scratch_shapes=[
            pltpu.VMEM(router.shape, router.dtype),
            pltpu.VMEM((slots, down_step, width), expert_down.dtype),
            pltpu.VMEM((tokens, columns), jnp.bfloat16),
            pltpu.SemaphoreType.DMA,
            pltpu.SemaphoreType.DMA((slots,)),
        ],
        compiler_params=params(25),
        cost_estimate=cost(10**11),
        name="mlp",
    )(
        routes, projected, hidden, ln_gain, router, shared_up, shared_down, expert_up, expert_down
    )


def fast_body(
    query, key_new, value_new, key_cache, value_cache, lengths, hidden, routes, w_out,
    ln_gain, router, shared_up, shared_down, expert_up, expert_down,
):
    width = query.shape[1]
    blocks = width // LANES
    cache_len = key_cache.shape[1]
    tokens = routes.shape[0]
    in_hbm = functools.partial(pltpu.with_memory_space_constraint, memory_space=pltpu.HBM)
    query, key_new, value_new, key_cache, value_cache, hidden = map(
        in_hbm, (query, key_new, value_new, key_cache, value_cache, hidden)
    )
    in_vmem = functools.partial(pltpu.with_memory_space_constraint, memory_space=pltpu.VMEM)
    router, expert_down = map(in_hbm, (router.T, expert_down))
    shared_up, shared_down, expert_up = map(in_vmem, (shared_up, shared_down, expert_up))
    row = pltpu.VMEM((1, width), jnp.bfloat16)
    cache = pltpu.VMEM((cache_len, width), jnp.bfloat16)
    message = pl.pallas_call(
        attend_kernel,
        out_shape=jax.ShapeDtypeStruct((tokens, 2 * blocks, LANES), jnp.bfloat16),
        in_specs=[SMEM] + [HBM] * 6,
        out_specs=VMEM,
        scratch_shapes=[row] * 4 + [cache] * 2 + [pltpu.SemaphoreType.DMA((6,))],
        compiler_params=params(4),
        cost_estimate=cost(10**11),
        name="attend",
    )(lengths, query, key_new, value_new, key_cache, value_cache, hidden)
    gathered = lax.all_to_all(message, "expert", 0, 0)
    message, every_hidden = pl.pallas_call(
        project_kernel,
        out_shape=(
            jax.ShapeDtypeStruct((tokens, tokens, LANES), jnp.bfloat16),
            jax.ShapeDtypeStruct((tokens, width), jnp.bfloat16),
        ),
        in_specs=[VMEM] * 4,
        out_specs=(VMEM, VMEM),
        compiler_params=params(4),
        cost_estimate=cost(10**11),
        name="project",
    )(gathered, w_out, shared_up, shared_down)
    every_projected = lax.all_to_all(message, "expert", 0, 0)
    terms, own = mlp(
        routes, in_vmem(every_projected), in_vmem(every_hidden), ln_gain.reshape(blocks, LANES), router,
        shared_up, shared_down, expert_up, expert_down,
    )
    terms = lax.all_to_all(terms, "expert", 0, 0)
    return pl.pallas_call(
        combine_kernel,
        out_shape=jax.ShapeDtypeStruct((1, width), jnp.bfloat16),
        in_specs=[VMEM] * 2,
        out_specs=VMEM,
        compiler_params=params(2),
        name="combine",
    )(terms, own)


def fits_fast(
    query, key_new, value_new, key_cache, value_cache, lengths, hidden, routes, w_out, *rest
):
    tokens = routes.shape[0]
    return (
        query.shape[0] == 1
        and HEAD_DIM == LANES
        and w_out.shape[1] == LANES
        and tokens * LANES == query.shape[1]
        and rest[4].shape[1] % FF == 0
    )


def pick_body(*args):
    return fast_body(*args) if fits_fast(*args) else body(*args)


def solution(mesh):
    placed = (
        P(("group", "expert"), None),
        P(("group", "expert"), None),
        P(("group", "expert"), None),
        P(("group", "expert"), None, None),
        P(("group", "expert"), None, None),
        P(("group", "expert")),
        P(("group", "expert"), None),
        P("group"),
        P(None, "expert"),
        P(),
        P(),
        P(None, "expert"),
        P("expert", None),
        P(None, "expert"),
        P("expert", None),
    )
    return jax.shard_map(
        pick_body, mesh=mesh, in_specs=placed, out_specs=P(("group", "expert"), None), check_vma=False
    )
```

```python
import functools
import math

import jax
import jax.numpy as jnp
from jax import lax
from jax.experimental import pallas as pl
from jax.experimental.pallas import tpu as pltpu
from jax.sharding import PartitionSpec as P

D = 2048
HEADS = 16
HEAD_DIM = 128
FF = 4096
EXPERTS = 32


def attend(query, key_new, value_new, key_cache, value_cache, lengths):
    seq_count = query.shape[0]
    cache_len = key_cache.shape[1]
    scale_factor = 1.0 / math.sqrt(HEAD_DIM)
    head_query = query.reshape(seq_count, HEADS, HEAD_DIM)
    head_keys = key_cache.reshape(seq_count, cache_len, HEADS, HEAD_DIM)
    head_values = value_cache.reshape(seq_count, cache_len, HEADS, HEAD_DIM)
    scores = (
        jnp.einsum("shd,schd->shc", head_query, head_keys, preferred_element_type=jnp.float32)
        * scale_factor
    )
    own_score = (
        jnp.einsum(
            "shd,shd->sh",
            head_query,
            key_new.reshape(seq_count, HEADS, HEAD_DIM),
            preferred_element_type=jnp.float32,
        )
        * scale_factor
    )
    positions = jnp.arange(cache_len, dtype=jnp.int32)
    scores = jnp.where(positions[None, None, :] < lengths[:, None, None], scores, -1e30)
    top_score = jnp.maximum(jnp.max(scores, axis=2), own_score)
    weights = jnp.exp(scores - top_score[:, :, None])
    own_weight = jnp.exp(own_score - top_score)
    normalizer = jnp.sum(weights, axis=2) + own_weight
    weights = (weights / normalizer[:, :, None]).astype(jnp.bfloat16)
    own_weight = (own_weight / normalizer).astype(jnp.bfloat16)
    mixed_values = jnp.einsum(
        "shc,schd->shd", weights, head_values, preferred_element_type=jnp.float32
    )
    mixed_values = mixed_values + own_weight.astype(jnp.float32)[:, :, None] * value_new.reshape(
        seq_count, HEADS, HEAD_DIM
    ).astype(jnp.float32)
    return mixed_values.reshape(seq_count, HEADS * HEAD_DIM).astype(jnp.bfloat16)


def body(
    query,
    key_new,
    value_new,
    key_cache,
    value_cache,
    lengths,
    hidden,
    routes,
    w_out,
    ln_gain,
    router,
    shared_up,
    shared_down,
    expert_up,
    expert_down,
):
    seq_count = query.shape[0]
    attended = attend(query, key_new, value_new, key_cache, value_cache, lengths)
    every_attended, every_hidden = (
        lax.all_gather(attended, "expert", axis=0, tiled=True),
        lax.all_gather(hidden, "expert", axis=0, tiled=True),
    )
    projected = jnp.dot(every_attended, w_out, preferred_element_type=jnp.float32).astype(
        jnp.bfloat16
    )
    every_projected = lax.all_gather(projected, "expert", axis=1, tiled=True)
    residual = every_hidden.astype(jnp.float32) + every_projected.astype(jnp.float32)
    centered = residual - jnp.mean(residual, axis=1, keepdims=True)
    variance = jnp.mean(centered * centered, axis=1, keepdims=True)
    normed = (
        centered / jnp.sqrt(jnp.maximum(variance, 0.25)) * ln_gain.astype(jnp.float32)
    ).astype(jnp.bfloat16)
    logits = jnp.dot(normed, router, preferred_element_type=jnp.float32)
    all_experts = jnp.arange(EXPERTS, dtype=jnp.int32)
    chosen = jnp.sum(jnp.where(routes[:, None] == all_experts[None, :], logits, 0.0), axis=1)
    gate_value = jax.nn.sigmoid(chosen)
    shared_hidden = jax.nn.gelu(
        jnp.dot(normed, shared_up, preferred_element_type=jnp.float32), approximate=True
    ).astype(jnp.bfloat16)
    total_tokens = routes.shape[0]
    capacity = 4 * total_tokens // EXPERTS
    column_count = expert_up.shape[1]
    local_units = min(column_count, FF)
    local_experts = column_count // local_units
    device_index = lax.axis_index("expert")
    first_expert = device_index * column_count // FF
    expert_ids = first_expert + jnp.arange(local_experts, dtype=jnp.int32)
    member = routes[:, None] == expert_ids[None, :]
    slot_rank = jnp.cumsum(member.astype(jnp.int32), axis=0) - 1
    slot_ids = jnp.arange(capacity, dtype=jnp.int32)
    placed = member[:, :, None] & (slot_rank[:, :, None] == slot_ids[None, None, :])
    picked = jnp.einsum(
        "skc,sd->kcd", placed.astype(jnp.bfloat16), normed, preferred_element_type=jnp.float32
    ).astype(jnp.bfloat16)
    up_local = expert_up.reshape(D, local_experts, local_units)
    inner_act = jax.nn.gelu(
        jnp.einsum("kcd,dkf->kcf", picked, up_local, preferred_element_type=jnp.float32),
        approximate=True,
    ).astype(jnp.bfloat16)
    down_local = expert_down.reshape(local_experts, local_units, D)
    result = jnp.einsum("kcf,kfd->kcd", inner_act, down_local, preferred_element_type=jnp.float32)
    spread = placed.astype(jnp.float32) * gate_value[:, None, None]
    summed = lax.psum_scatter(
        jnp.dot(shared_hidden, shared_down, preferred_element_type=jnp.float32)
        + jnp.einsum("skc,kcd->sd", spread, result, precision=lax.Precision.HIGHEST),
        "expert",
        scatter_dimension=0,
        tiled=True,
    )
    own_residual = lax.dynamic_slice_in_dim(residual, device_index * seq_count, seq_count, 0)
    combined = own_residual + summed
    return combined.astype(jnp.bfloat16)


LANES = 128
HEAD_ROWS = 1024


def per_head(row, heads):
    index = lax.broadcasted_iota(jnp.int32, (heads, LANES), 0)
    out = jnp.zeros((heads, LANES), jnp.float32)
    for head in range(heads):
        piece = row[:, head * LANES : (head + 1) * LANES]
        out = jnp.where(index == head, piece, out)
    return out


def attend_kernel(
    axis, lengths, query, key_new, value_new, keys, values, hidden, expert_down, out, down_head,
    query_buf, key_new_buf, value_new_buf, hidden_buf, keys_buf, values_buf, sems,
):
    half = expert_down.shape[0] // lax.axis_size(axis)
    first = pl.multiple_of(lax.axis_index(axis) * half, LANES)
    copies = [
        pltpu.make_async_copy(source, target, sems.at[slot])
        for slot, (source, target) in enumerate(
            (
                (query, query_buf),
                (keys.at[0], keys_buf),
                (key_new, key_new_buf),
                (values.at[0], values_buf),
                (value_new, value_new_buf),
                (hidden, hidden_buf),
                (expert_down.at[pl.ds(first, down_head.shape[0])], down_head),
            )
        )
    ]
    for copy in copies:
        copy.start()
    cache_len, width = keys_buf.shape
    heads = width // HEAD_DIM
    scale_factor = 1.0 / math.sqrt(HEAD_DIM)
    valid = lengths[0]
    copies[0].wait()
    lane_head = lax.broadcasted_iota(jnp.int32, (heads, width), 1) // HEAD_DIM
    row_head = lax.broadcasted_iota(jnp.int32, (heads, width), 0)
    head_query = jnp.where(lane_head == row_head, query_buf[...].astype(jnp.float32), 0.0)
    copies[2].wait()
    own_score = (
        jnp.sum(head_query * key_new_buf[...].astype(jnp.float32), axis=1, keepdims=True)
        * scale_factor
    )
    copies[1].wait()
    scores = (
        lax.dot_general(
            head_query.astype(jnp.bfloat16),
            keys_buf[...],
            (((1,), (1,)), ((), ())),
            preferred_element_type=jnp.float32,
        )
        * scale_factor
    )
    positions = lax.broadcasted_iota(jnp.int32, (heads, cache_len), 1)
    scores = jnp.where(positions < valid, scores, -1e30)
    top_score = jnp.maximum(jnp.max(scores, axis=1, keepdims=True), own_score)
    weights = jnp.exp(scores - top_score)
    own_weight = jnp.exp(own_score - top_score)
    normalizer = jnp.sum(weights, axis=1, keepdims=True) + own_weight
    weights = (weights / normalizer).astype(jnp.bfloat16)
    own_weight = (own_weight / normalizer).astype(jnp.bfloat16).astype(jnp.float32)
    copies[3].wait()
    mixed = jnp.dot(weights, values_buf[...], preferred_element_type=jnp.float32)
    copies[4].wait()
    copies[5].wait()
    own_value = per_head(value_new_buf[...].astype(jnp.float32), heads)
    attended = (per_head(mixed, heads) + own_weight * own_value).astype(jnp.bfloat16)
    pieces = per_head(hidden_buf[...].astype(jnp.float32), heads)
    out[:, :heads, :] = jnp.broadcast_to(attended[None], (out.shape[0], heads, LANES))
    extra = out.shape[1] - heads
    for peer in range(out.shape[0]):
        piece = jnp.broadcast_to(pieces[peer : peer + 1], (extra, LANES))
        out[peer, heads:, :] = piece.astype(jnp.bfloat16)
    copies[6].wait()


def project_kernel(gathered, w_out, shared_up, shared_down, out):
    tokens, rows, _ = gathered.shape
    heads = w_out.shape[0] // LANES
    flat = gathered[...].reshape(tokens * rows, LANES)
    shape = (tokens * (heads + 1), tokens * rows)
    target = lax.broadcasted_iota(jnp.int32, shape, 0)
    source = lax.broadcasted_iota(jnp.int32, shape, 1)
    wanted = (target % tokens) * rows + target // tokens
    swap = jnp.where(source == wanted, 1.0, 0.0).astype(jnp.bfloat16)
    swapped = jnp.dot(swap, flat, preferred_element_type=jnp.float32)
    blocks = [swapped[row * tokens : (row + 1) * tokens] for row in range(heads + 1)]
    attended = jnp.concatenate(blocks[:heads], axis=1).astype(jnp.bfloat16)
    projected = jnp.dot(attended, w_out[...], preferred_element_type=jnp.float32)
    residual = blocks[heads] + projected.astype(jnp.bfloat16).astype(jnp.float32)
    out[...] = jnp.broadcast_to(residual.astype(jnp.bfloat16)[None], out.shape)


def gelu(value):
    return jax.nn.gelu(value, approximate=True).astype(jnp.bfloat16)


def mlp_kernel(
    axes, up_step, down_step,
    routes_in, residuals, ln_gain, router, shared_up, shared_down, expert_up, down_head,
    expert_down, out, own_out,
    routes, router_buf, down_buf, act_buf, terms_buf, sems, down_sems,
):
    group, member = (lax.axis_index(axis) for axis in axes)
    groups, members = (lax.axis_size(axis) for axis in axes)
    group_tokens = routes.shape[0]
    tokens = groups * group_tokens
    width = shared_up.shape[0]
    blocks = width // LANES
    columns = expert_up.shape[1] // groups
    first_column = group * columns
    head = down_head.shape[0]
    down_count = (columns - head) // down_step

    def part(start, size):
        return pl.ds(pl.multiple_of(start, LANES), size)

    def down_copy(index):
        return pltpu.make_async_copy(
            expert_down.at[part(first_column + head + index * down_step, down_step)],
            down_buf.at[index],
            down_sems.at[index],
        )

    routes_copy = pltpu.make_async_copy(routes_in, routes, sems.at[0])
    router_copy = pltpu.make_async_copy(router, router_buf, sems.at[1])
    routes_copy.start()
    router_copy.start()

    @pl.loop(0, down_count)
    def _(index):
        down_copy(index).start()

    residual = jnp.concatenate(
        [
            jnp.concatenate(
                [residuals[base + block].astype(jnp.float32) for block in range(blocks)], axis=1
            )
            for base in range(0, groups * members, members)
        ],
        axis=0,
    )
    centered = residual - jnp.mean(residual, axis=1, keepdims=True)
    variance = jnp.mean(centered * centered, axis=1, keepdims=True)
    gain = ln_gain[...].astype(jnp.float32)
    gain = jnp.concatenate([gain[block : block + 1] for block in range(blocks)], axis=1)
    normed = (centered / jnp.sqrt(jnp.maximum(variance, 0.25)) * gain).astype(jnp.bfloat16)
    for step in range(columns // up_step):
        act_buf[:, step * up_step : (step + 1) * up_step] = gelu(
            jnp.dot(
                normed,
                expert_up[:, part(first_column + step * up_step, up_step)],
                preferred_element_type=jnp.float32,
            )
        )

    here_normed = normed[:group_tokens]
    for other in range(1, groups):
        rows = normed[other * group_tokens : (other + 1) * group_tokens]
        here_normed = jnp.where(group == other, rows, here_normed)
    shared_act = gelu(jnp.dot(here_normed, shared_up[...], preferred_element_type=jnp.float32))
    shared = jnp.dot(shared_act, shared_down[...], preferred_element_type=jnp.float32)
    token = lax.broadcasted_iota(jnp.int32, (tokens, width), 0)
    own = jnp.where(token == group * group_tokens + member, residual, 0.0)
    own_out[:blocks] = per_head(jnp.sum(own, axis=0, keepdims=True), blocks)

    router_copy.wait()
    routes_copy.wait()
    logits = lax.dot_general(
        here_normed, router_buf[...], (((1,), (1,)), ((), ())), preferred_element_type=jnp.float32
    )
    token_column = lax.broadcasted_iota(jnp.int32, (group_tokens, 1), 0)
    route = jnp.zeros((group_tokens, 1), jnp.int32)
    for index in range(group_tokens):
        route = jnp.where(token_column == index, routes[index], route)
    expert_lane = lax.broadcasted_iota(jnp.int32, logits.shape, 1)
    chosen = jnp.sum(jnp.where(expert_lane == route, logits, 0.0), axis=1, keepdims=True)
    gate = jax.nn.sigmoid(chosen)
    own_gate = jnp.sum(jnp.where(token_column == member, gate, 0.0), axis=0, keepdims=True)
    own_route = jnp.sum(jnp.where(token_column == member, route, 0), axis=0, keepdims=True)
    holder = lax.rem(own_route, groups)
    own_holder = holder * members + own_route // groups
    away = jnp.where(holder == group, 0.0, own_gate)
    source = lax.broadcasted_iota(jnp.int32, (groups * members, LANES), 0)
    own_out[blocks:] = jnp.where(
        source // members == group, 1.0, jnp.where(source == own_holder, away, 0.0)
    )

    sums = jnp.dot(act_buf[:, :head], down_head[...], preferred_element_type=jnp.float32)
    for index in range(down_count):
        down_copy(index).wait()
        at = slice(head + index * down_step, head + (index + 1) * down_step)
        sums = sums + jnp.dot(
            act_buf[:, at], down_buf[index], preferred_element_type=jnp.float32
        )
    here_gate = jnp.where(route == member * groups + group, gate, 0.0)
    parts = []
    for other in range(groups):
        rows = sums[other * group_tokens : (other + 1) * group_tokens]
        parts.append(jnp.where(group == other, shared + here_gate * rows, rows))
    total = jnp.concatenate(parts, axis=0)
    for block in range(blocks):
        terms_buf[:, block, :] = total[:, block * LANES : (block + 1) * LANES]
    out[...] = terms_buf[...].astype(out.dtype)


def combine_kernel(terms, own, out):
    blocks = terms.shape[1]
    total = own[:blocks]
    for index in range(terms.shape[0]):
        scale = own[blocks + index : blocks + index + 1]
        total = total + scale * terms[index].astype(jnp.float32)
    for block in range(blocks):
        out[:, block * LANES : (block + 1) * LANES] = total[block : block + 1].astype(out.dtype)


VMEM = pl.BlockSpec(memory_space=pltpu.VMEM)
SMEM = pl.BlockSpec(memory_space=pltpu.SMEM)
HBM = pl.BlockSpec(memory_space=pltpu.HBM)


def params(megabytes):
    return pltpu.CompilerParams(vmem_limit_bytes=megabytes << 20)


def cost(flops):
    return pl.CostEstimate(flops=flops, bytes_accessed=flops >> 8, transcendentals=0)


def mlp(
    routes, residuals, ln_gain, router, shared_up, shared_down, expert_up, down_head, expert_down
):
    tokens = residuals.shape[0]
    width, columns = expert_up.shape
    blocks = width // LANES
    columns = columns // lax.axis_size("group")
    down_step, up_step = 512, 1024
    down_count = (columns - down_head.shape[0]) // down_step
    return pl.pallas_call(
        functools.partial(mlp_kernel, ("group", "expert"), up_step, down_step),
        out_shape=(
            pltpu.VMEM((tokens, blocks, LANES), jnp.bfloat16),
            pltpu.VMEM((blocks + tokens, LANES), jnp.float32),
        ),
        in_specs=[HBM, VMEM, VMEM, HBM, VMEM, VMEM, VMEM, VMEM, HBM],
        out_specs=(VMEM, VMEM),
        scratch_shapes=[
            pltpu.SMEM(routes.shape, routes.dtype),
            pltpu.VMEM(router.shape, router.dtype),
            pltpu.VMEM((down_count, down_step, width), expert_down.dtype),
            pltpu.VMEM((tokens, columns), jnp.bfloat16),
            pltpu.VMEM((tokens, blocks, LANES), jnp.float32),
            pltpu.SemaphoreType.DMA((2,)),
            pltpu.SemaphoreType.DMA((down_count,)),
        ],
        compiler_params=params(17),
        cost_estimate=cost(10**11),
        name="mlp",
    )(
        routes, residuals, ln_gain, router, shared_up, shared_down, expert_up, down_head,
        expert_down,
    )


def fast_body(
    query, key_new, value_new, key_cache, value_cache, lengths, hidden, routes, w_out,
    ln_gain, router, shared_up, shared_down, expert_up, expert_down,
):
    width = query.shape[1]
    blocks = width // LANES
    cache_len = key_cache.shape[1]
    tokens = routes.shape[0]
    both = ("group", "expert")
    groups = lax.axis_size("group")
    in_hbm = functools.partial(pltpu.with_memory_space_constraint, memory_space=pltpu.HBM)
    in_vmem = functools.partial(pltpu.with_memory_space_constraint, memory_space=pltpu.VMEM)
    query, key_new, value_new, key_cache, value_cache, hidden = map(
        in_hbm, (query, key_new, value_new, key_cache, value_cache, hidden)
    )
    router, expert_down = map(in_hbm, (router.T, expert_down))
    shared_up, shared_down, expert_up = map(in_vmem, (shared_up, shared_down, expert_up))
    row = pltpu.VMEM((1, width), jnp.bfloat16)
    cache = pltpu.VMEM((cache_len, width), jnp.bfloat16)
    message, down_head = pl.pallas_call(
        functools.partial(attend_kernel, "group"),
        out_shape=(
            pltpu.VMEM((tokens, blocks + 8, LANES), jnp.bfloat16),
            pltpu.VMEM((HEAD_ROWS, width), expert_down.dtype),
        ),
        in_specs=[SMEM] + [HBM] * 7,
        out_specs=(VMEM, VMEM),
        scratch_shapes=[row] * 4 + [cache] * 2 + [pltpu.SemaphoreType.DMA((7,))],
        compiler_params=params(4),
        cost_estimate=cost(10**11),
        name="attend",
    )(lengths, query, key_new, value_new, key_cache, value_cache, hidden, expert_down)
    gathered = lax.all_to_all(message, "expert", 0, 0)
    message = pl.pallas_call(
        project_kernel,
        out_shape=jax.ShapeDtypeStruct((groups * tokens, tokens, LANES), jnp.bfloat16),
        in_specs=[VMEM] * 4,
        out_specs=VMEM,
        compiler_params=params(4),
        cost_estimate=cost(10**11),
        name="project",
    )(gathered, w_out, shared_up, shared_down)
    residuals = lax.all_to_all(message, both, 0, 0)
    terms, own = mlp(
        in_hbm(routes), in_vmem(residuals), in_vmem(ln_gain.reshape(blocks, LANES)), router,
        shared_up, shared_down, expert_up, in_vmem(down_head), expert_down,
    )
    terms = lax.all_to_all(terms, both, 0, 0)
    return pl.pallas_call(
        combine_kernel,
        out_shape=jax.ShapeDtypeStruct((1, width), jnp.bfloat16),
        in_specs=[VMEM, VMEM],
        out_specs=VMEM,
        compiler_params=params(2),
        name="combine",
    )(terms, own)


def fits_fast(
    query, key_new, value_new, key_cache, value_cache, lengths, hidden, routes, w_out, *rest
):
    tokens = routes.shape[0]
    return (
        query.shape[0] == 1
        and HEAD_DIM == LANES
        and w_out.shape[1] == LANES
        and tokens * LANES == query.shape[1]
        and lax.axis_size("group") == 2
        and rest[4].shape[1] == 2 * FF
    )


def pick_body(*args):
    return fast_body(*args) if fits_fast(*args) else body(*args)


def solution(mesh):
    placed = (
        P(("group", "expert"), None),
        P(("group", "expert"), None),
        P(("group", "expert"), None),
        P(("group", "expert"), None, None),
        P(("group", "expert"), None, None),
        P(("group", "expert")),
        P(("group", "expert"), None),
        P("group"),
        P(None, "expert"),
        P(),
        P(),
        P(None, "expert"),
        P("expert", None),
        P(None, "expert"),
        P("expert", None),
    )
    return jax.shard_map(
        pick_body, mesh=mesh, in_specs=placed, out_specs=P(("group", "expert"), None), check_vma=False
    )
```

```python
import functools
import math

import jax
import jax.numpy as jnp
from jax import lax
from jax.experimental import pallas as pl
from jax.experimental.pallas import tpu as pltpu
from jax.sharding import PartitionSpec as P

D = 2048
HEADS = 16
HEAD_DIM = 128
FF = 4096
EXPERTS = 32


def attend(query, key_new, value_new, key_cache, value_cache, lengths):
    seq_count = query.shape[0]
    cache_len = key_cache.shape[1]
    scale_factor = 1.0 / math.sqrt(HEAD_DIM)
    head_query = query.reshape(seq_count, HEADS, HEAD_DIM)
    head_keys = key_cache.reshape(seq_count, cache_len, HEADS, HEAD_DIM)
    head_values = value_cache.reshape(seq_count, cache_len, HEADS, HEAD_DIM)
    scores = (
        jnp.einsum("shd,schd->shc", head_query, head_keys, preferred_element_type=jnp.float32)
        * scale_factor
    )
    own_score = (
        jnp.einsum(
            "shd,shd->sh",
            head_query,
            key_new.reshape(seq_count, HEADS, HEAD_DIM),
            preferred_element_type=jnp.float32,
        )
        * scale_factor
    )
    positions = jnp.arange(cache_len, dtype=jnp.int32)
    scores = jnp.where(positions[None, None, :] < lengths[:, None, None], scores, -1e30)
    top_score = jnp.maximum(jnp.max(scores, axis=2), own_score)
    weights = jnp.exp(scores - top_score[:, :, None])
    own_weight = jnp.exp(own_score - top_score)
    normalizer = jnp.sum(weights, axis=2) + own_weight
    weights = (weights / normalizer[:, :, None]).astype(jnp.bfloat16)
    own_weight = (own_weight / normalizer).astype(jnp.bfloat16)
    mixed_values = jnp.einsum(
        "shc,schd->shd", weights, head_values, preferred_element_type=jnp.float32
    )
    mixed_values = mixed_values + own_weight.astype(jnp.float32)[:, :, None] * value_new.reshape(
        seq_count, HEADS, HEAD_DIM
    ).astype(jnp.float32)
    return mixed_values.reshape(seq_count, HEADS * HEAD_DIM).astype(jnp.bfloat16)


def body(
    query,
    key_new,
    value_new,
    key_cache,
    value_cache,
    lengths,
    hidden,
    routes,
    w_out,
    ln_gain,
    router,
    shared_up,
    shared_down,
    expert_up,
    expert_down,
):
    seq_count = query.shape[0]
    attended = attend(query, key_new, value_new, key_cache, value_cache, lengths)
    every_attended, every_hidden = (
        lax.all_gather(attended, "expert", axis=0, tiled=True),
        lax.all_gather(hidden, "expert", axis=0, tiled=True),
    )
    projected = jnp.dot(every_attended, w_out, preferred_element_type=jnp.float32).astype(
        jnp.bfloat16
    )
    every_projected = lax.all_gather(projected, "expert", axis=1, tiled=True)
    residual = every_hidden.astype(jnp.float32) + every_projected.astype(jnp.float32)
    centered = residual - jnp.mean(residual, axis=1, keepdims=True)
    variance = jnp.mean(centered * centered, axis=1, keepdims=True)
    normed = (
        centered / jnp.sqrt(jnp.maximum(variance, 0.25)) * ln_gain.astype(jnp.float32)
    ).astype(jnp.bfloat16)
    logits = jnp.dot(normed, router, preferred_element_type=jnp.float32)
    all_experts = jnp.arange(EXPERTS, dtype=jnp.int32)
    chosen = jnp.sum(jnp.where(routes[:, None] == all_experts[None, :], logits, 0.0), axis=1)
    gate_value = jax.nn.sigmoid(chosen)
    shared_hidden = jax.nn.gelu(
        jnp.dot(normed, shared_up, preferred_element_type=jnp.float32), approximate=True
    ).astype(jnp.bfloat16)
    total_tokens = routes.shape[0]
    capacity = 4 * total_tokens // EXPERTS
    column_count = expert_up.shape[1]
    local_units = min(column_count, FF)
    local_experts = column_count // local_units
    device_index = lax.axis_index("expert")
    first_expert = device_index * column_count // FF
    expert_ids = first_expert + jnp.arange(local_experts, dtype=jnp.int32)
    member = routes[:, None] == expert_ids[None, :]
    slot_rank = jnp.cumsum(member.astype(jnp.int32), axis=0) - 1
    slot_ids = jnp.arange(capacity, dtype=jnp.int32)
    placed = member[:, :, None] & (slot_rank[:, :, None] == slot_ids[None, None, :])
    picked = jnp.einsum(
        "skc,sd->kcd", placed.astype(jnp.bfloat16), normed, preferred_element_type=jnp.float32
    ).astype(jnp.bfloat16)
    up_local = expert_up.reshape(D, local_experts, local_units)
    inner_act = jax.nn.gelu(
        jnp.einsum("kcd,dkf->kcf", picked, up_local, preferred_element_type=jnp.float32),
        approximate=True,
    ).astype(jnp.bfloat16)
    down_local = expert_down.reshape(local_experts, local_units, D)
    result = jnp.einsum("kcf,kfd->kcd", inner_act, down_local, preferred_element_type=jnp.float32)
    spread = placed.astype(jnp.float32) * gate_value[:, None, None]
    summed = lax.psum_scatter(
        jnp.dot(shared_hidden, shared_down, preferred_element_type=jnp.float32)
        + jnp.einsum("skc,kcd->sd", spread, result, precision=lax.Precision.HIGHEST),
        "expert",
        scatter_dimension=0,
        tiled=True,
    )
    own_residual = lax.dynamic_slice_in_dim(residual, device_index * seq_count, seq_count, 0)
    combined = own_residual + summed
    return combined.astype(jnp.bfloat16)


LANES = 128
HEAD_ROWS = 512
PIECES = (1536, 1024, 512, 512)


def per_head(row, heads):
    index = lax.broadcasted_iota(jnp.int32, (heads, LANES), 0)
    out = jnp.zeros((heads, LANES), jnp.float32)
    for head in range(heads):
        piece = row[:, head * LANES : (head + 1) * LANES]
        out = jnp.where(index == head, piece, out)
    return out


def attend_kernel(
    axis, lengths, query, key_new, value_new, keys, values, hidden, expert_down, out, down_head,
    query_buf, key_new_buf, value_new_buf, hidden_buf, keys_buf, values_buf, sems,
):
    half = expert_down.shape[0] // lax.axis_size(axis)
    first = pl.multiple_of(lax.axis_index(axis) * half, LANES)
    copies = [
        pltpu.make_async_copy(source, target, sems.at[slot])
        for slot, (source, target) in enumerate(
            (
                (query, query_buf),
                (keys.at[0], keys_buf),
                (key_new, key_new_buf),
                (values.at[0], values_buf),
                (value_new, value_new_buf),
                (hidden, hidden_buf),
                (expert_down.at[pl.ds(first, down_head.shape[0])], down_head),
            )
        )
    ]
    for copy in copies:
        copy.start()
    cache_len, width = keys_buf.shape
    heads = width // HEAD_DIM
    scale_factor = 1.0 / math.sqrt(HEAD_DIM)
    valid = lengths[0]
    copies[0].wait()
    lane_head = lax.broadcasted_iota(jnp.int32, (heads, width), 1) // HEAD_DIM
    row_head = lax.broadcasted_iota(jnp.int32, (heads, width), 0)
    head_query = jnp.where(lane_head == row_head, query_buf[...].astype(jnp.float32), 0.0)
    copies[2].wait()
    own_score = (
        jnp.sum(head_query * key_new_buf[...].astype(jnp.float32), axis=1, keepdims=True)
        * scale_factor
    )
    copies[1].wait()
    scores = (
        lax.dot_general(
            head_query.astype(jnp.bfloat16),
            keys_buf[...],
            (((1,), (1,)), ((), ())),
            preferred_element_type=jnp.float32,
        )
        * scale_factor
    )
    positions = lax.broadcasted_iota(jnp.int32, (heads, cache_len), 1)
    scores = jnp.where(positions < valid, scores, -1e30)
    top_score = jnp.maximum(jnp.max(scores, axis=1, keepdims=True), own_score)
    weights = jnp.exp(scores - top_score)
    own_weight = jnp.exp(own_score - top_score)
    normalizer = jnp.sum(weights, axis=1, keepdims=True) + own_weight
    weights = (weights / normalizer).astype(jnp.bfloat16)
    own_weight = (own_weight / normalizer).astype(jnp.bfloat16).astype(jnp.float32)
    copies[3].wait()
    mixed = jnp.dot(weights, values_buf[...], preferred_element_type=jnp.float32)
    copies[4].wait()
    copies[5].wait()
    own_value = per_head(value_new_buf[...].astype(jnp.float32), heads)
    attended = (per_head(mixed, heads) + own_weight * own_value).astype(jnp.bfloat16)
    pieces = per_head(hidden_buf[...].astype(jnp.float32), heads)
    out[:, :heads, :] = jnp.broadcast_to(attended[None], (out.shape[0], heads, LANES))
    extra = out.shape[1] - heads
    for peer in range(out.shape[0]):
        piece = jnp.broadcast_to(pieces[peer : peer + 1], (extra, LANES))
        out[peer, heads:, :] = piece.astype(jnp.bfloat16)
    copies[6].wait()


def project_kernel(gathered, w_out, shared_up, shared_down, out):
    tokens, rows, _ = gathered.shape
    heads = w_out.shape[0] // LANES
    flat = gathered[...].reshape(tokens * rows, LANES)
    shape = (tokens * (heads + 1), tokens * rows)
    target = lax.broadcasted_iota(jnp.int32, shape, 0)
    source = lax.broadcasted_iota(jnp.int32, shape, 1)
    wanted = (target % tokens) * rows + target // tokens
    swap = jnp.where(source == wanted, 1.0, 0.0).astype(jnp.bfloat16)
    swapped = jnp.dot(swap, flat, preferred_element_type=jnp.float32)
    blocks = [swapped[row * tokens : (row + 1) * tokens] for row in range(heads + 1)]
    attended = jnp.concatenate(blocks[:heads], axis=1).astype(jnp.bfloat16)
    projected = jnp.dot(attended, w_out[...], preferred_element_type=jnp.float32)
    residual = blocks[heads] + projected.astype(jnp.bfloat16).astype(jnp.float32)
    out[...] = jnp.broadcast_to(residual.astype(jnp.bfloat16)[None], out.shape)


def gelu(value):
    return jax.nn.gelu(value, approximate=True).astype(jnp.bfloat16)


def part_of(group, members):
    return pl.ds(group * members, members)


def mlp_kernel(
    axes, up_step, pieces,
    routes_in, residuals, ln_gain, router, shared_up, shared_down, expert_up, down_head,
    expert_down, out, own_out,
    routes, down_buf, act_buf, terms_buf, routes_sem, down_sems,
):
    group, member = (lax.axis_index(axis) for axis in axes)
    groups, members = (lax.axis_size(axis) for axis in axes)
    group_tokens = routes.shape[0]
    tokens = groups * group_tokens
    width = shared_up.shape[0]
    blocks = width // LANES
    columns = expert_up.shape[1] // groups
    first_column = group * columns
    head = down_head.shape[0]
    step_rows = pieces[-1]

    def part(start, size):
        return pl.ds(pl.multiple_of(start, LANES), size)

    def down_copy(index):
        rows = part(index * step_rows, step_rows)
        return pltpu.make_async_copy(
            expert_down.at[part(first_column + head + index * step_rows, step_rows)],
            down_buf.at[rows],
            down_sems.at[index],
        )

    routes_copy = pltpu.make_async_copy(routes_in, routes, routes_sem)
    routes_copy.start()

    @pl.loop(0, (columns - head) // step_rows)
    def _(index):
        down_copy(index).start()

    residual = jnp.concatenate(
        [
            jnp.concatenate(
                [residuals[base + block].astype(jnp.float32) for block in range(blocks)], axis=1
            )
            for base in range(0, groups * members, members)
        ],
        axis=0,
    )
    mean = jnp.mean(residual, axis=1, keepdims=True)
    centered = residual - mean
    variance = jnp.mean(centered * centered, axis=1, keepdims=True)
    gain = ln_gain[...].astype(jnp.float32)
    gain = jnp.concatenate([gain[block : block + 1] for block in range(blocks)], axis=1)
    normed = (centered * (1.0 / jnp.sqrt(jnp.maximum(variance, 0.25))) * gain).astype(
        jnp.bfloat16
    )
    for step in range(columns // up_step):
        act_buf[:, step * up_step : (step + 1) * up_step] = gelu(
            jnp.dot(
                normed,
                expert_up[:, part(first_column + step * up_step, up_step)],
                preferred_element_type=jnp.float32,
            )
        )

    here_normed = normed[:group_tokens]
    for other in range(1, groups):
        rows = normed[other * group_tokens : (other + 1) * group_tokens]
        here_normed = jnp.where(group == other, rows, here_normed)
    shared_act = gelu(jnp.dot(here_normed, shared_up[...], preferred_element_type=jnp.float32))
    shared = jnp.dot(shared_act, shared_down[...], preferred_element_type=jnp.float32)
    logits = lax.dot_general(
        here_normed, router[...], (((1,), (1,)), ((), ())), preferred_element_type=jnp.float32
    )
    here = residuals[part_of(group, members)].astype(jnp.float32)
    token = lax.broadcasted_iota(jnp.int32, here.shape, 1)
    own_out[:blocks] = jnp.sum(jnp.where(token == member, here, 0.0), axis=1)
    sums = jnp.dot(act_buf[:, :head], down_head[...], preferred_element_type=jnp.float32)

    routes_copy.wait()
    token_column = lax.broadcasted_iota(jnp.int32, (group_tokens, 1), 0)
    route = jnp.zeros((group_tokens, 1), jnp.int32)
    for index in range(group_tokens):
        route = jnp.where(token_column == index, routes[index], route)
    expert_lane = lax.broadcasted_iota(jnp.int32, logits.shape, 1)
    chosen = jnp.sum(jnp.where(expert_lane == route, logits, 0.0), axis=1, keepdims=True)
    gate = jax.nn.sigmoid(chosen)
    own_gate = jnp.sum(jnp.where(token_column == member, gate, 0.0), axis=0, keepdims=True)
    own_route = jnp.sum(jnp.where(token_column == member, route, 0), axis=0, keepdims=True)
    holder = lax.rem(own_route, groups)
    own_holder = holder * members + own_route // groups
    away = jnp.where(holder == group, 0.0, own_gate)
    source = lax.broadcasted_iota(jnp.int32, (groups * members, LANES), 0)
    own_out[blocks:] = jnp.where(
        source // members == group, 1.0, jnp.where(source == own_holder, away, 0.0)
    )

    first = 0
    for size in pieces:
        for index in range(first // step_rows, (first + size) // step_rows):
            down_copy(index).wait()
        sums = sums + jnp.dot(
            act_buf[:, head + first : head + first + size],
            down_buf[first : first + size],
            preferred_element_type=jnp.float32,
        )
        first += size
    here_gate = jnp.where(route == member * groups + group, gate, 0.0)
    parts = []
    for other in range(groups):
        rows = sums[other * group_tokens : (other + 1) * group_tokens]
        parts.append(jnp.where(group == other, shared + here_gate * rows, rows))
    total = jnp.concatenate(parts, axis=0)
    for block in range(blocks):
        terms_buf[:, block, :] = total[:, block * LANES : (block + 1) * LANES]
    out[...] = terms_buf[...].astype(out.dtype)


def combine_kernel(terms, own, out):
    blocks = terms.shape[1]
    total = own[:blocks]
    for index in range(terms.shape[0]):
        scale = own[blocks + index : blocks + index + 1]
        total = total + scale * terms[index].astype(jnp.float32)
    for block in range(blocks):
        out[:, block * LANES : (block + 1) * LANES] = total[block : block + 1].astype(out.dtype)


VMEM = pl.BlockSpec(memory_space=pltpu.VMEM)
SMEM = pl.BlockSpec(memory_space=pltpu.SMEM)
HBM = pl.BlockSpec(memory_space=pltpu.HBM)


def params(megabytes):
    return pltpu.CompilerParams(vmem_limit_bytes=megabytes << 20)


def cost(flops):
    return pl.CostEstimate(flops=flops, bytes_accessed=flops >> 8, transcendentals=0)


def mlp(
    routes, residuals, ln_gain, router, shared_up, shared_down, expert_up, down_head, expert_down
):
    tokens = residuals.shape[0]
    width, columns = expert_up.shape
    blocks = width // LANES
    columns = columns // lax.axis_size("group")
    up_step, pieces = 1024, PIECES
    rows = columns - down_head.shape[0]
    return pl.pallas_call(
        functools.partial(mlp_kernel, ("group", "expert"), up_step, pieces),
        out_shape=(
            pltpu.VMEM((tokens, blocks, LANES), jnp.bfloat16),
            pltpu.VMEM((blocks + tokens, LANES), jnp.float32),
        ),
        in_specs=[HBM, VMEM, VMEM, VMEM, VMEM, VMEM, VMEM, VMEM, HBM],
        out_specs=(VMEM, VMEM),
        scratch_shapes=[
            pltpu.SMEM(routes.shape, routes.dtype),
            pltpu.VMEM((rows, width), expert_down.dtype),
            pltpu.VMEM((tokens, columns), jnp.bfloat16),
            pltpu.VMEM((tokens, blocks, LANES), jnp.float32),
            pltpu.SemaphoreType.DMA,
            pltpu.SemaphoreType.DMA((rows // pieces[-1],)),
        ],
        compiler_params=params(19),
        cost_estimate=cost(10**11),
        name="mlp",
    )(
        routes, residuals, ln_gain, router, shared_up, shared_down, expert_up, down_head,
        expert_down,
    )


def fast_body(
    query, key_new, value_new, key_cache, value_cache, lengths, hidden, routes, w_out,
    ln_gain, router, shared_up, shared_down, expert_up, expert_down,
):
    width = query.shape[1]
    blocks = width // LANES
    cache_len = key_cache.shape[1]
    tokens = routes.shape[0]
    both = ("group", "expert")
    groups = lax.axis_size("group")
    in_hbm = functools.partial(pltpu.with_memory_space_constraint, memory_space=pltpu.HBM)
    in_vmem = functools.partial(pltpu.with_memory_space_constraint, memory_space=pltpu.VMEM)
    query, key_new, value_new, key_cache, value_cache, hidden = map(
        in_hbm, (query, key_new, value_new, key_cache, value_cache, hidden)
    )
    expert_down = in_hbm(expert_down)
    shared_up, shared_down, expert_up, router = map(
        in_vmem, (shared_up, shared_down, expert_up, router.T)
    )
    row = pltpu.VMEM((1, width), jnp.bfloat16)
    cache = pltpu.VMEM((cache_len, width), jnp.bfloat16)
    message, down_head = pl.pallas_call(
        functools.partial(attend_kernel, "group"),
        out_shape=(
            pltpu.VMEM((tokens, blocks + 8, LANES), jnp.bfloat16),
            pltpu.VMEM((HEAD_ROWS, width), expert_down.dtype),
        ),
        in_specs=[SMEM] + [HBM] * 7,
        out_specs=(VMEM, VMEM),
        scratch_shapes=[row] * 4 + [cache] * 2 + [pltpu.SemaphoreType.DMA((7,))],
        compiler_params=params(4),
        cost_estimate=cost(10**11),
        name="attend",
    )(lengths, query, key_new, value_new, key_cache, value_cache, hidden, expert_down)
    gathered = lax.all_to_all(message, "expert", 0, 0)
    message = pl.pallas_call(
        project_kernel,
        out_shape=jax.ShapeDtypeStruct((groups * tokens, tokens, LANES), jnp.bfloat16),
        in_specs=[VMEM] * 4,
        out_specs=VMEM,
        compiler_params=params(4),
        cost_estimate=cost(10**11),
        name="project",
    )(gathered, w_out, shared_up, shared_down)
    residuals = lax.all_to_all(message, both, 0, 0)
    terms, own = mlp(
        in_hbm(routes), in_vmem(residuals), in_vmem(ln_gain.reshape(blocks, LANES)), router,
        shared_up, shared_down, expert_up, in_vmem(down_head), expert_down,
    )
    terms = lax.all_to_all(terms, both, 0, 0)
    return pl.pallas_call(
        combine_kernel,
        out_shape=jax.ShapeDtypeStruct((1, width), jnp.bfloat16),
        in_specs=[VMEM, VMEM],
        out_specs=VMEM,
        compiler_params=params(2),
        name="combine",
    )(terms, own)


def fits_fast(
    query, key_new, value_new, key_cache, value_cache, lengths, hidden, routes, w_out, *rest
):
    tokens = routes.shape[0]
    return (
        query.shape[0] == 1
        and HEAD_DIM == LANES
        and w_out.shape[1] == LANES
        and tokens * LANES == query.shape[1]
        and lax.axis_size("group") == 2
        and rest[4].shape[1] == 2 * FF
    )


def pick_body(*args):
    return fast_body(*args) if fits_fast(*args) else body(*args)


def solution(mesh):
    placed = (
        P(("group", "expert"), None),
        P(("group", "expert"), None),
        P(("group", "expert"), None),
        P(("group", "expert"), None, None),
        P(("group", "expert"), None, None),
        P(("group", "expert")),
        P(("group", "expert"), None),
        P("group"),
        P(None, "expert"),
        P(),
        P(),
        P(None, "expert"),
        P("expert", None),
        P(None, "expert"),
        P("expert", None),
    )
    return jax.shard_map(
        pick_body, mesh=mesh, in_specs=placed, out_specs=P(("group", "expert"), None), check_vma=False
    )
```

```python
import functools
import math

import jax
import jax.numpy as jnp
from jax import lax
from jax.experimental import pallas as pl
from jax.experimental.pallas import tpu as pltpu
from jax.sharding import PartitionSpec as P

D = 2048
HEADS = 16
HEAD_DIM = 128
FF = 4096
EXPERTS = 32


def attend(query, key_new, value_new, key_cache, value_cache, lengths):
    seq_count = query.shape[0]
    cache_len = key_cache.shape[1]
    scale_factor = 1.0 / math.sqrt(HEAD_DIM)
    head_query = query.reshape(seq_count, HEADS, HEAD_DIM)
    head_keys = key_cache.reshape(seq_count, cache_len, HEADS, HEAD_DIM)
    head_values = value_cache.reshape(seq_count, cache_len, HEADS, HEAD_DIM)
    scores = (
        jnp.einsum("shd,schd->shc", head_query, head_keys, preferred_element_type=jnp.float32)
        * scale_factor
    )
    own_score = (
        jnp.einsum(
            "shd,shd->sh",
            head_query,
            key_new.reshape(seq_count, HEADS, HEAD_DIM),
            preferred_element_type=jnp.float32,
        )
        * scale_factor
    )
    positions = jnp.arange(cache_len, dtype=jnp.int32)
    scores = jnp.where(positions[None, None, :] < lengths[:, None, None], scores, -1e30)
    top_score = jnp.maximum(jnp.max(scores, axis=2), own_score)
    weights = jnp.exp(scores - top_score[:, :, None])
    own_weight = jnp.exp(own_score - top_score)
    normalizer = jnp.sum(weights, axis=2) + own_weight
    weights = (weights / normalizer[:, :, None]).astype(jnp.bfloat16)
    own_weight = (own_weight / normalizer).astype(jnp.bfloat16)
    mixed_values = jnp.einsum(
        "shc,schd->shd", weights, head_values, preferred_element_type=jnp.float32
    )
    mixed_values = mixed_values + own_weight.astype(jnp.float32)[:, :, None] * value_new.reshape(
        seq_count, HEADS, HEAD_DIM
    ).astype(jnp.float32)
    return mixed_values.reshape(seq_count, HEADS * HEAD_DIM).astype(jnp.bfloat16)


def body(
    query,
    key_new,
    value_new,
    key_cache,
    value_cache,
    lengths,
    hidden,
    routes,
    w_out,
    ln_gain,
    router,
    shared_up,
    shared_down,
    expert_up,
    expert_down,
):
    seq_count = query.shape[0]
    attended = attend(query, key_new, value_new, key_cache, value_cache, lengths)
    every_attended, every_hidden = (
        lax.all_gather(attended, "expert", axis=0, tiled=True),
        lax.all_gather(hidden, "expert", axis=0, tiled=True),
    )
    projected = jnp.dot(every_attended, w_out, preferred_element_type=jnp.float32).astype(
        jnp.bfloat16
    )
    every_projected = lax.all_gather(projected, "expert", axis=1, tiled=True)
    residual = every_hidden.astype(jnp.float32) + every_projected.astype(jnp.float32)
    centered = residual - jnp.mean(residual, axis=1, keepdims=True)
    variance = jnp.mean(centered * centered, axis=1, keepdims=True)
    normed = (
        centered / jnp.sqrt(jnp.maximum(variance, 0.25)) * ln_gain.astype(jnp.float32)
    ).astype(jnp.bfloat16)
    logits = jnp.dot(normed, router, preferred_element_type=jnp.float32)
    all_experts = jnp.arange(EXPERTS, dtype=jnp.int32)
    chosen = jnp.sum(jnp.where(routes[:, None] == all_experts[None, :], logits, 0.0), axis=1)
    gate_value = jax.nn.sigmoid(chosen)
    shared_hidden = jax.nn.gelu(
        jnp.dot(normed, shared_up, preferred_element_type=jnp.float32), approximate=True
    ).astype(jnp.bfloat16)
    total_tokens = routes.shape[0]
    capacity = 4 * total_tokens // EXPERTS
    column_count = expert_up.shape[1]
    local_units = min(column_count, FF)
    local_experts = column_count // local_units
    device_index = lax.axis_index("expert")
    first_expert = device_index * column_count // FF
    expert_ids = first_expert + jnp.arange(local_experts, dtype=jnp.int32)
    member = routes[:, None] == expert_ids[None, :]
    slot_rank = jnp.cumsum(member.astype(jnp.int32), axis=0) - 1
    slot_ids = jnp.arange(capacity, dtype=jnp.int32)
    placed = member[:, :, None] & (slot_rank[:, :, None] == slot_ids[None, None, :])
    picked = jnp.einsum(
        "skc,sd->kcd", placed.astype(jnp.bfloat16), normed, preferred_element_type=jnp.float32
    ).astype(jnp.bfloat16)
    up_local = expert_up.reshape(D, local_experts, local_units)
    inner_act = jax.nn.gelu(
        jnp.einsum("kcd,dkf->kcf", picked, up_local, preferred_element_type=jnp.float32),
        approximate=True,
    ).astype(jnp.bfloat16)
    down_local = expert_down.reshape(local_experts, local_units, D)
    result = jnp.einsum("kcf,kfd->kcd", inner_act, down_local, preferred_element_type=jnp.float32)
    spread = placed.astype(jnp.float32) * gate_value[:, None, None]
    summed = lax.psum_scatter(
        jnp.dot(shared_hidden, shared_down, preferred_element_type=jnp.float32)
        + jnp.einsum("skc,kcd->sd", spread, result, precision=lax.Precision.HIGHEST),
        "expert",
        scatter_dimension=0,
        tiled=True,
    )
    own_residual = lax.dynamic_slice_in_dim(residual, device_index * seq_count, seq_count, 0)
    combined = own_residual + summed
    return combined.astype(jnp.bfloat16)


LANES = 128
HEAD_ROWS = 512
PIECES = (1536, 1024, 512, 512)


def per_head(row, heads):
    index = lax.broadcasted_iota(jnp.int32, (heads, LANES), 0)
    out = jnp.zeros((heads, LANES), jnp.float32)
    for head in range(heads):
        piece = row[:, head * LANES : (head + 1) * LANES]
        out = jnp.where(index == head, piece, out)
    return out


def attend_kernel(
    axis, lengths, query, key_new, value_new, keys, values, hidden, expert_down, out, down_head,
    query_buf, key_new_buf, value_new_buf, hidden_buf, keys_buf, values_buf, sems,
):
    half = expert_down.shape[0] // lax.axis_size(axis)
    first = pl.multiple_of(lax.axis_index(axis) * half, LANES)
    copies = [
        pltpu.make_async_copy(source, target, sems.at[slot])
        for slot, (source, target) in enumerate(
            (
                (query, query_buf),
                (keys.at[0], keys_buf),
                (key_new, key_new_buf),
                (values.at[0], values_buf),
                (value_new, value_new_buf),
                (hidden, hidden_buf),
                (expert_down.at[pl.ds(first, down_head.shape[0])], down_head),
            )
        )
    ]
    for copy in copies:
        copy.start()
    cache_len, width = keys_buf.shape
    heads = width // HEAD_DIM
    scale_factor = 1.0 / math.sqrt(HEAD_DIM)
    valid = lengths[0]
    copies[0].wait()
    lane_head = lax.broadcasted_iota(jnp.int32, (heads, width), 1) // HEAD_DIM
    row_head = lax.broadcasted_iota(jnp.int32, (heads, width), 0)
    head_query = jnp.where(lane_head == row_head, query_buf[...].astype(jnp.float32), 0.0)
    copies[2].wait()
    own_score = (
        jnp.sum(head_query * key_new_buf[...].astype(jnp.float32), axis=1, keepdims=True)
        * scale_factor
    )
    copies[1].wait()
    scores = (
        lax.dot_general(
            head_query.astype(jnp.bfloat16),
            keys_buf[...],
            (((1,), (1,)), ((), ())),
            preferred_element_type=jnp.float32,
        )
        * scale_factor
    )
    positions = lax.broadcasted_iota(jnp.int32, (heads, cache_len), 1)
    scores = jnp.where(positions < valid, scores, -1e30)
    top_score = jnp.maximum(jnp.max(scores, axis=1, keepdims=True), own_score)
    weights = jnp.exp(scores - top_score)
    own_weight = jnp.exp(own_score - top_score)
    normalizer = jnp.sum(weights, axis=1, keepdims=True) + own_weight
    weights = (weights / normalizer).astype(jnp.bfloat16)
    own_weight = (own_weight / normalizer).astype(jnp.bfloat16).astype(jnp.float32)
    copies[3].wait()
    mixed = jnp.dot(weights, values_buf[...], preferred_element_type=jnp.float32)
    copies[4].wait()
    copies[5].wait()
    own_value = per_head(value_new_buf[...].astype(jnp.float32), heads)
    attended = (per_head(mixed, heads) + own_weight * own_value).astype(jnp.bfloat16)
    pieces = per_head(hidden_buf[...].astype(jnp.float32), heads)
    out[:, :heads, :] = jnp.broadcast_to(attended[None], (out.shape[0], heads, LANES))
    extra = out.shape[1] - heads
    for peer in range(out.shape[0]):
        piece = jnp.broadcast_to(pieces[peer : peer + 1], (extra, LANES))
        out[peer, heads:, :] = piece.astype(jnp.bfloat16)
    copies[6].wait()


def hand_on_kernel(source, out):
    out[0, 0:8] = source[0, 0:8]


def project_kernel(gathered, w_out, shared_up, shared_down, out):
    tokens, rows, _ = gathered.shape
    heads = w_out.shape[0] // LANES
    flat = gathered[...].reshape(tokens * rows, LANES)
    shape = (tokens * (heads + 1), tokens * rows)
    target = lax.broadcasted_iota(jnp.int32, shape, 0)
    source = lax.broadcasted_iota(jnp.int32, shape, 1)
    wanted = (target % tokens) * rows + target // tokens
    swap = jnp.where(source == wanted, 1.0, 0.0).astype(jnp.bfloat16)
    swapped = jnp.dot(swap, flat, preferred_element_type=jnp.float32)
    blocks = [swapped[row * tokens : (row + 1) * tokens] for row in range(heads + 1)]
    attended = jnp.concatenate(blocks[:heads], axis=1).astype(jnp.bfloat16)
    projected = jnp.dot(attended, w_out[...], preferred_element_type=jnp.float32)
    residual = blocks[heads] + projected.astype(jnp.bfloat16).astype(jnp.float32)
    out[...] = jnp.broadcast_to(residual.astype(jnp.bfloat16)[None], out.shape)


def gelu(value):
    return jax.nn.gelu(value, approximate=True).astype(jnp.bfloat16)


TILE = 256


def stream(jobs):
    lanes = [[job for job in jobs if job[0] == unit] for unit in range(2)]
    longest = max(len(lane) for lane in lanes)
    for step in range(longest + 1):
        for unit, lane in enumerate(lanes):
            if step < len(lane):
                pltpu.matmul_push_rhs(
                    lane[step][3](), staging_register=step % 2, mxu_index=unit
                )
        for unit, lane in enumerate(lanes):
            if 0 < step <= len(lane):
                _, acc, rows, _, after = lane[step - 1]
                pltpu.matmul_acc_lhs(acc, rows(), load_staged_rhs=(step - 1) % 2)
                if after is not None:
                    after()


def part_of(group, members):
    return pl.ds(group * members, members)


def mlp_kernel(axes, pieces, *refs):
    tokens, blocks = refs[9].shape[0], refs[9].shape[1]
    wide = blocks * LANES // TILE // 2

    def accumulators(rows, count):
        return tuple((pltpu.ACC(q)((rows, TILE), jnp.float32),) * count for q in range(2))

    pl.run_scoped(
        lambda *accs: mlp_body(axes, pieces, accs, *refs),
        accumulators(tokens, 2),
        accumulators(tokens, wide),
        accumulators(tokens // 2, wide),
    )


def mlp_body(
    axes, pieces, accs,
    routes_in, residuals, ln_gain, router, shared_up, shared_down, expert_up, down_head,
    expert_down, out, own_out,
    routes, down_buf, act_buf, terms_buf, routes_sem, down_sems,
):
    group, member = (lax.axis_index(axis) for axis in axes)
    groups, members = (lax.axis_size(axis) for axis in axes)
    group_tokens = routes.shape[0]
    tokens = groups * group_tokens
    width = shared_up.shape[0]
    blocks = width // LANES
    columns = expert_up.shape[1] // groups
    first_column = group * columns
    head = down_head.shape[0]
    step_rows = pieces[-1]

    def part(start, size):
        return pl.ds(pl.multiple_of(start, LANES), size)

    def down_copy(index):
        rows = part(index * step_rows, step_rows)
        return pltpu.make_async_copy(
            expert_down.at[part(first_column + head + index * step_rows, step_rows)],
            down_buf.at[rows],
            down_sems.at[index],
        )

    routes_copy = pltpu.make_async_copy(routes_in, routes, routes_sem)
    routes_copy.start()

    @pl.loop(0, (columns - head) // step_rows)
    def _(index):
        down_copy(index).start()

    residual = jnp.concatenate(
        [
            jnp.concatenate(
                [residuals[base + block].astype(jnp.float32) for block in range(blocks)], axis=1
            )
            for base in range(0, groups * members, members)
        ],
        axis=0,
    )
    mean = jnp.mean(residual, axis=1, keepdims=True)
    centered = residual - mean
    variance = jnp.mean(centered * centered, axis=1, keepdims=True)
    gain = ln_gain[...].astype(jnp.float32)
    gain = jnp.concatenate([gain[block : block + 1] for block in range(blocks)], axis=1)
    normed = (centered * (1.0 / jnp.sqrt(jnp.maximum(variance, 0.25))) * gain).astype(
        jnp.bfloat16
    )
    depth = width // TILE
    up_accs, down_accs, small_accs = accs
    for kind in accs:
        for unit_accs in kind:
            for acc in unit_accs:
                pltpu.matmul_pop(acc)

    def wide(start):
        return part(start, TILE)

    def up_jobs(column, spare):
        unit = column % 2
        acc = up_accs[unit][spare]

        def finish():
            act_buf[:, column * TILE : (column + 1) * TILE] = gelu(pltpu.matmul_pop(acc))

        def job(k):
            return (
                unit,
                acc,
                lambda: normed[:, k * TILE : (k + 1) * TILE],
                lambda: expert_up[
                    k * TILE : (k + 1) * TILE, wide(first_column + column * TILE)
                ],
                finish if k == depth - 1 else None,
            )

        return [job(k) for k in range(depth)]

    stream([job for column in range(columns // TILE) for job in up_jobs(column, column // 2 % 2)])

    here_normed = normed[:group_tokens]
    for other in range(1, groups):
        rows = normed[other * group_tokens : (other + 1) * group_tokens]
        here_normed = jnp.where(group == other, rows, here_normed)
    shared_units = shared_up.shape[1]
    shared_act = []

    def shared_up_job(column, k):
        acc = small_accs[column % 2][column // 2]
        return (
            column % 2,
            acc,
            lambda: here_normed[:, k * TILE : (k + 1) * TILE],
            lambda: shared_up[k * TILE : (k + 1) * TILE, column * TILE : (column + 1) * TILE],
            (lambda: shared_act.append(gelu(pltpu.matmul_pop(acc)))) if k == depth - 1 else None,
        )

    stream([shared_up_job(c, k) for c in range(shared_units // TILE) for k in range(depth)])
    shared_parts = []

    def shared_down_job(column, k):
        acc = small_accs[column % 2][column // 2]
        last = k == shared_units // TILE - 1
        return (
            column % 2,
            acc,
            lambda: shared_act[k],
            lambda: shared_down[k * TILE : (k + 1) * TILE, column * TILE : (column + 1) * TILE],
            (lambda: shared_parts.append(pltpu.matmul_pop(acc))) if last else None,
        )

    stream(
        [shared_down_job(c, k) for c in range(depth) for k in range(shared_units // TILE)]
    )
    shared = jnp.concatenate(shared_parts, axis=1)

    def down_jobs(rows_ref, act_start, start, size):
        def job(column, k):
            return (
                column % 2,
                down_accs[column % 2][column // 2],
                lambda: act_buf[:, act_start + k * TILE : act_start + (k + 1) * TILE],
                lambda: rows_ref[
                    start + k * TILE : start + (k + 1) * TILE,
                    column * TILE : (column + 1) * TILE,
                ],
                None,
            )

        return [job(c, k) for c in range(depth) for k in range(size // TILE)]

    here = residuals[part_of(group, members)].astype(jnp.float32)
    token = lax.broadcasted_iota(jnp.int32, here.shape, 1)
    own_out[:blocks] = jnp.sum(jnp.where(token == member, here, 0.0), axis=1)
    stream(down_jobs(down_head, 0, 0, head))

    routes_copy.wait()
    token_column = lax.broadcasted_iota(jnp.int32, (group_tokens, 1), 0)
    route = jnp.zeros((group_tokens, 1), jnp.int32)
    for index in range(group_tokens):
        route = jnp.where(token_column == index, routes[index], route)
    router_rows = router[...].astype(jnp.float32)
    expert_row = lax.broadcasted_iota(jnp.int32, router_rows.shape, 0)

    def gate_for(expert):
        picked = jnp.sum(jnp.where(expert_row == expert, router_rows, 0.0), axis=0, keepdims=True)
        products = here_normed.astype(jnp.float32) * picked
        return jax.nn.sigmoid(jnp.sum(products, axis=1, keepdims=True))

    here_expert = member * groups + group
    own_gate = jnp.sum(
        jnp.where(token_column == member, gate_for(routes[member]), 0.0), axis=0, keepdims=True
    )
    own_route = jnp.sum(jnp.where(token_column == member, route, 0), axis=0, keepdims=True)
    holder = lax.rem(own_route, groups)
    own_holder = holder * members + own_route // groups
    away = jnp.where(holder == group, 0.0, own_gate)
    source = lax.broadcasted_iota(jnp.int32, (groups * members, LANES), 0)
    own_out[blocks:] = jnp.where(
        source // members == group, 1.0, jnp.where(source == own_holder, away, 0.0)
    )

    first = 0
    for size in pieces:
        for index in range(first // step_rows, (first + size) // step_rows):
            down_copy(index).wait()
        stream(down_jobs(down_buf, head + first, first, size))
        first += size
    sums = jnp.concatenate(
        [pltpu.matmul_pop(down_accs[column % 2][column // 2]) for column in range(depth)], axis=1
    )
    here_gate = jnp.where(route == here_expert, gate_for(here_expert), 0.0)
    parts = []
    for other in range(groups):
        rows = sums[other * group_tokens : (other + 1) * group_tokens]
        parts.append(jnp.where(group == other, shared + here_gate * rows, rows))
    total = jnp.concatenate(parts, axis=0)
    for block in range(blocks):
        terms_buf[:, block, :] = total[:, block * LANES : (block + 1) * LANES]
    out[...] = terms_buf[...].astype(out.dtype)


def combine_kernel(terms, own, out):
    blocks = terms.shape[1]
    total = own[:blocks]
    for index in range(terms.shape[0]):
        scale = own[blocks + index : blocks + index + 1]
        total = total + scale * terms[index].astype(jnp.float32)
    for block in range(blocks):
        out[:, block * LANES : (block + 1) * LANES] = total[block : block + 1].astype(out.dtype)


VMEM = pl.BlockSpec(memory_space=pltpu.VMEM)
SMEM = pl.BlockSpec(memory_space=pltpu.SMEM)
HBM = pl.BlockSpec(memory_space=pltpu.HBM)


def params(megabytes):
    return pltpu.CompilerParams(vmem_limit_bytes=megabytes << 20)


def cost(flops):
    return pl.CostEstimate(flops=flops, bytes_accessed=flops >> 8, transcendentals=0)


def mlp(
    routes, residuals, ln_gain, router, shared_up, shared_down, expert_up, down_head, expert_down
):
    tokens = residuals.shape[0]
    width, columns = expert_up.shape
    blocks = width // LANES
    columns = columns // lax.axis_size("group")
    pieces = PIECES
    rows = columns - down_head.shape[0]
    return pl.pallas_call(
        functools.partial(mlp_kernel, ("group", "expert"), pieces),
        out_shape=(
            pltpu.VMEM((tokens, blocks, LANES), jnp.bfloat16),
            pltpu.VMEM((blocks + tokens, LANES), jnp.float32),
        ),
        in_specs=[HBM, VMEM, VMEM, VMEM, VMEM, VMEM, VMEM, VMEM, HBM],
        out_specs=(VMEM, VMEM),
        scratch_shapes=[
            pltpu.SMEM(routes.shape, routes.dtype),
            pltpu.VMEM((rows, width), expert_down.dtype),
            pltpu.VMEM((tokens, columns), jnp.bfloat16),
            pltpu.VMEM((tokens, blocks, LANES), jnp.float32),
            pltpu.SemaphoreType.DMA,
            pltpu.SemaphoreType.DMA((rows // pieces[-1],)),
        ],
        compiler_params=params(19),
        cost_estimate=cost(10**11),
        name="mlp",
    )(
        routes, residuals, ln_gain, router, shared_up, shared_down, expert_up, down_head,
        expert_down,
    )


def fast_body(
    query, key_new, value_new, key_cache, value_cache, lengths, hidden, routes, w_out,
    ln_gain, router, shared_up, shared_down, expert_up, expert_down,
):
    width = query.shape[1]
    blocks = width // LANES
    cache_len = key_cache.shape[1]
    tokens = routes.shape[0]
    both = ("group", "expert")
    groups = lax.axis_size("group")
    in_hbm = functools.partial(pltpu.with_memory_space_constraint, memory_space=pltpu.HBM)
    in_vmem = functools.partial(pltpu.with_memory_space_constraint, memory_space=pltpu.VMEM)
    query, key_new, value_new, key_cache, value_cache, hidden = map(
        in_hbm, (query, key_new, value_new, key_cache, value_cache, hidden)
    )
    expert_down = in_hbm(expert_down)
    shared_up, shared_down, expert_up, router = map(
        in_vmem, (shared_up, shared_down, expert_up, router.T)
    )
    row = pltpu.VMEM((1, width), jnp.bfloat16)
    cache = pltpu.VMEM((cache_len, width), jnp.bfloat16)
    message, down_head = pl.pallas_call(
        functools.partial(attend_kernel, "group"),
        out_shape=(
            pltpu.VMEM((tokens, blocks + 8, LANES), jnp.bfloat16),
            pltpu.VMEM((HEAD_ROWS, width), expert_down.dtype),
        ),
        in_specs=[SMEM] + [HBM] * 7,
        out_specs=(VMEM, VMEM),
        scratch_shapes=[row] * 4 + [cache] * 2 + [pltpu.SemaphoreType.DMA((7,))],
        compiler_params=params(4),
        cost_estimate=cost(10**6),
        name="attend",
    )(lengths, query, key_new, value_new, key_cache, value_cache, hidden, expert_down)
    message = pl.pallas_call(
        hand_on_kernel,
        out_shape=pltpu.VMEM(message.shape, message.dtype),
        in_specs=[VMEM],
        out_specs=VMEM,
        input_output_aliases={0: 0},
        compiler_params=params(2),
        cost_estimate=cost(10**12),
        name="hand_on",
    )(message)
    gathered = lax.all_to_all(message, "expert", 0, 0)
    message = pl.pallas_call(
        project_kernel,
        out_shape=jax.ShapeDtypeStruct((groups * tokens, tokens, LANES), jnp.bfloat16),
        in_specs=[VMEM] * 4,
        out_specs=VMEM,
        compiler_params=params(4),
        cost_estimate=cost(10**11),
        name="project",
    )(gathered, w_out, shared_up, shared_down)
    residuals = lax.all_to_all(message, both, 0, 0)
    terms, own = mlp(
        in_hbm(routes), in_vmem(residuals), in_vmem(ln_gain.reshape(blocks, LANES)), router,
        shared_up, shared_down, expert_up, in_vmem(down_head), expert_down,
    )
    terms = lax.all_to_all(terms, both, 0, 0)
    return pl.pallas_call(
        combine_kernel,
        out_shape=jax.ShapeDtypeStruct((1, width), jnp.bfloat16),
        in_specs=[VMEM, VMEM],
        out_specs=VMEM,
        compiler_params=params(2),
        name="combine",
    )(terms, own)


def fits_fast(
    query, key_new, value_new, key_cache, value_cache, lengths, hidden, routes, w_out, *rest
):
    tokens = routes.shape[0]
    return (
        query.shape[0] == 1
        and HEAD_DIM == LANES
        and w_out.shape[1] == LANES
        and tokens * LANES == query.shape[1]
        and lax.axis_size("group") == 2
        and rest[4].shape[1] == 2 * FF
    )


def pick_body(*args):
    return fast_body(*args) if fits_fast(*args) else body(*args)


def solution(mesh):
    placed = (
        P(("group", "expert"), None),
        P(("group", "expert"), None),
        P(("group", "expert"), None),
        P(("group", "expert"), None, None),
        P(("group", "expert"), None, None),
        P(("group", "expert")),
        P(("group", "expert"), None),
        P("group"),
        P(None, "expert"),
        P(),
        P(),
        P(None, "expert"),
        P("expert", None),
        P(None, "expert"),
        P("expert", None),
    )
    return jax.shard_map(
        pick_body, mesh=mesh, in_specs=placed, out_specs=P(("group", "expert"), None), check_vma=False
    )
```
